32 devices in a mesh: dp: 8 (over z, x), seq: 4 (over y, core).
Axes of the slice: x: 2, y: 2, z: 4, core: 2. Of those that a mesh axis runs over, the one named last changes fastest.
Arguments:
- tokens: int32 [2, 16, 2048], P(None, 'dp', 'seq'), may hold values from 0 to 30521
- segment_ends: int32 [2, 16, 2], P(None, 'dp'), may hold values from 128 to 2048, as said below
- word_table: bfloat16 [30522, 128], replicated, may hold values from -6 to 6
- trigram_conv: bfloat16 [384, 512], replicated, may hold values from -0.3125 to 0.3125
- position_table: bfloat16 [2048, 512], P('seq'), may hold values from -3 to 3
- segment_table: bfloat16 [2, 512], replicated, may hold values from -3 to 3
- embed_scalars: float32 [2, 512], replicated, may hold values from 0.5 to 1.5
- teacher_enter: bfloat16 [512, 1024], replicated, may hold values from -0.25 to 0.25
- teacher_attention: bfloat16 [1024, 3072], replicated, may hold values from -0.1875 to 0.1875
- teacher_combine: bfloat16 [1024, 1024], replicated, may hold values from -1.5 to 1.5
- teacher_expand: bfloat16 [1024, 4096], replicated, may hold values from -0.1875 to 0.1875
- teacher_reduce: bfloat16 [4096, 1024], replicated, may hold values from -0.09375 to 0.09375
- teacher_leave: bfloat16 [1024, 512], replicated, may hold values from -0.1875 to 0.1875
- teacher_scalars: float32 [16896], replicated, may hold values from 0.5 to 1.5
- narrowing: float32 [512, 128], replicated, may hold values from -0.25 to 0.25
- attention: float32 [128, 384], replicated, may hold values from -0.5 to 0.5
- combining: float32 [128, 128], replicated, may hold values from -4 to 4
- expanding: float32 [4, 128, 512], replicated, may hold values from -0.5 to 0.5
- reducing: float32 [4, 512, 128], replicated, may hold values from -0.25 to 0.25
- widening: float32 [128, 512], replicated, may hold values from -0.5 to 0.5
- scalars: float32 [6144], replicated, may hold values from 0.5 to 1
- moment_narrowing: float32 [512, 128], replicated, may hold values from -4.172325e-07 to 4.172325e-07
- moment_attention: float32 [128, 384], replicated, may hold values from -4.172325e-07 to 4.172325e-07
- moment_combining: float32 [128, 128], replicated, may hold values from -4.172325e-07 to 4.172325e-07
- moment_expanding: float32 [4, 128, 512], replicated, may hold values from -4.172325e-07 to 4.172325e-07
- moment_reducing: float32 [4, 512, 128], replicated, may hold values from -4.172325e-07 to 4.172325e-07
- moment_widening: float32 [128, 512], replicated, may hold values from -4.172325e-07 to 4.172325e-07
- moment_scalars: float32 [6144], replicated, may hold values from -1.66893e-06 to 1.66893e-06
- square_narrowing: float32 [512, 128], replicated, may hold values from 1.7193002e-16 to 2.7508803e-15
- square_attention: float32 [128, 384], replicated, may hold values from 1.7193002e-16 to 2.7508803e-15
- square_combining: float32 [128, 128], replicated, may hold values from 1.7193002e-16 to 2.7508803e-15
- square_expanding: float32 [4, 128, 512], replicated, may hold values from 1.7193002e-16 to 2.7508803e-15
- square_reducing: float32 [4, 512, 128], replicated, may hold values from 1.7193002e-16 to 2.7508803e-15
- square_widening: float32 [128, 512], replicated, may hold values from 1.7193002e-16 to 2.7508803e-15
- square_scalars: float32 [6144], replicated, may hold values from 2.7508803e-15 to 4.4014085e-14
Outputs:
- weight_narrowing: float32 [512, 128], replicated
- weight_attention: float32 [128, 384], replicated
- weight_combining: float32 [128, 128], replicated
- weight_expanding: float32 [4, 128, 512], replicated
- weight_reducing: float32 [4, 512, 128], replicated
- weight_widening: float32 [128, 512], replicated
- weight_scalars: float32 [6144], replicated
- first_narrowing: float32 [512, 128], replicated
- first_attention: float32 [128, 384], replicated
- first_combining: float32 [128, 128], replicated
- first_expanding: float32 [4, 128, 512], replicated
- first_reducing: float32 [4, 512, 128], replicated
- first_widening: float32 [128, 512], replicated
- first_scalars: float32 [6144], replicated
- second_narrowing: float32 [512, 128], replicated
- second_attention: float32 [128, 384], replicated
- second_combining: float32 [128, 128], replicated
- second_expanding: float32 [4, 128, 512], replicated
- second_reducing: float32 [4, 512, 128], replicated
- second_widening: float32 [128, 512], replicated
- second_scalars: float32 [6144], replicated
- loss: float32 [1], replicated
- grad_norm: float32 [1], replicated
The draws below stay inside these ranges and needn't reach their ends.
Inputs may be any that keep to these rules, and one draw needn't show every extreme that they name: segment_ends[m, r, 0] < segment_ends[m, r, 1]; the last row of every micro-batch has no padding, segment_ends[m, 15, 1] = 2048.
All inputs are finite; a program needn't handle non-finite values.
Results may differ from the reference program's by a relative error of at most 0.0008.
The reference program's roundings to bfloat16 on the way (of `inputs`) count: a program that leaves them out, or rounds other values in their place, can miss the bound.
Values may be sent and summed in bfloat16 or wider, within the bound.
A program may use at most 448 MiB of HBM per device.

```python
import math
import jax
import jax.numpy as jnp
import numpy as np
from jax import lax

D_S = 512
B_S = 128
HEADS = 4
FF_S = 512
NFFN = 4
D_T = 1024
FF_T = 4096
EMB = 128
VOCAB = 30522
LEN = 2048
MB = 2
STEP = 10
ROWS = 16
HD_S = 32
HD_T = 256
SSMALL = 6144
TSMALL = 16896
NALL = 727040


def draw_segment_ends(key, part):
    first_key, second_key = jax.random.split(jax.random.fold_in(key, 11))
    rows = jnp.arange(ROWS, dtype=jnp.int32)
    lowest = LEN // 4 + rows * (LEN // 2) // max(ROWS - 1, 1)
    padding = lowest[None, :] + jax.random.randint(first_key, (MB, ROWS), 0, LEN // 4 + 1, dtype=jnp.int32)
    padding = jnp.minimum(padding, LEN)
    padding = jnp.where(rows[None, :] == ROWS - 1, LEN, padding)
    noise = jax.random.randint(second_key, (MB, ROWS), 0, 1 << 20, dtype=jnp.int32)
    second = noise % (padding // 2) + padding // 4
    return jnp.stack([second, padding], -1).astype(jnp.int32)


def set_ends(entries, key, smallest, largest):
    longest = entries.shape.index(max(entries.shape))
    spots = []
    for shift in (0, 1):
        where = [jax.random.randint(jax.random.fold_in(key, axis), (), 0, length) for axis, length in enumerate(entries.shape)]
        where[longest] = (where[longest] + shift) % entries.shape[longest]
        spots.append(tuple(where))
    return entries.at[spots[0]].set(smallest).at[spots[1]].set(largest)


def level_of(rng, dims, cuts, smallest, high):
    loudness = 1.0
    for dim, shards_of in cuts:
        draws = jax.random.uniform(jax.random.fold_in(jax.random.fold_in(rng, 6), dim), (shards_of,), jnp.float32, smallest / len(cuts), high / len(cuts))
        loudness = loudness * jnp.repeat(jnp.exp(draws), dims[dim] // shards_of).reshape((-1,) + (1,) * (len(dims) - 1 - dim))
    return loudness


def cumulative_ranks(number_of, skew):
    weights = [(1 << 20) // math.isqrt(grade ** skew) + 1 for grade in range(1, number_of + 1)]
    scale = 1 + sum(weights) // (1 << 30)
    return np.cumsum(np.array([max(1, weight // scale) for weight in weights]))


def skewed_ids(rng, dims, count, lean):
    listing = cumulative_ranks(count, lean)
    ticket = jax.random.randint(jax.random.fold_in(rng, 1), dims, 0, int(listing[count - 1]))
    rank = jnp.searchsorted(jnp.asarray(listing, jnp.int32), ticket, side="right")
    return jax.random.permutation(jax.random.fold_in(rng, 2), count)[rank].astype(jnp.int32)


def bell_draw(rng, shape, deviation, bound, cuts=(), kind=jnp.bfloat16):
    entries = jax.random.normal(rng, shape, jnp.float32) * deviation
    if len(cuts) > 0:
        entries = level_of(rng, shape, cuts, -0.22, 0.18) * entries
    return jnp.clip(entries, min=-bound, max=bound).astype(kind)


def setup_inputs(seed: int = 0) -> dict:
    key_list = jax.random.split(jax.random.key(seed), 36)
    return {
        "tokens": set_ends(skewed_ids(key_list[0], (MB, ROWS, LEN), VOCAB, 2), jax.random.fold_in(key_list[0], 3), 0, VOCAB - 1).astype(jnp.int32),
        "segment_ends": draw_segment_ends(jax.random.fold_in(key_list[35], 71), 0),
        "word_table": bell_draw(key_list[2], (VOCAB, EMB), 1.0, 6.0),
        "trigram_conv": bell_draw(key_list[3], (3 * EMB, D_S), (3 * EMB) ** -0.5, 0.3125),
        "position_table": bell_draw(key_list[4], (LEN, D_S), 0.5, 3.0, ((0, 4),)),
        "segment_table": bell_draw(key_list[5], (2, D_S), 0.5, 3.0),
        "embed_scalars": jnp.clip(1.0 + 0.1 * jax.random.normal(key_list[6], (2, D_S), jnp.float32), 0.5, 1.5),
        "teacher_enter": bell_draw(key_list[7], (D_S, D_T), D_S ** -0.5, 0.25),
        "teacher_attention": bell_draw(key_list[8], (D_T, 3 * D_T), D_T ** -0.5, 0.1875),
        "teacher_combine": bell_draw(key_list[9], (D_T, D_T), (max(1, D_T * 32 // LEN)) ** -0.5, 1.5),
        "teacher_expand": bell_draw(key_list[10], (D_T, FF_T), D_T ** -0.5, 0.1875),
        "teacher_reduce": bell_draw(key_list[11], (FF_T, D_T), FF_T ** -0.5, 0.09375),
        "teacher_leave": bell_draw(key_list[12], (D_T, D_S), D_T ** -0.5, 0.1875),
        "teacher_scalars": jnp.clip(1.0 + 0.1 * jax.random.normal(key_list[13], (TSMALL,), jnp.float32), 0.5, 1.5),
        "narrowing": bell_draw(key_list[14], (D_S, B_S), D_S ** -0.5, 0.25, (), jnp.float32),
        "attention": bell_draw(key_list[15], (B_S, 3 * B_S), B_S ** -0.5, 0.5, (), jnp.float32),
        "combining": bell_draw(key_list[16], (B_S, B_S), (max(1, B_S * 32 // LEN)) ** -0.5, 4.0, (), jnp.float32),
        "expanding": bell_draw(key_list[17], (NFFN, B_S, FF_S), B_S ** -0.5, 0.5, (), jnp.float32),
        "reducing": bell_draw(key_list[18], (NFFN, FF_S, B_S), FF_S ** -0.5, 0.25, (), jnp.float32),
        "widening": bell_draw(key_list[19], (B_S, D_S), B_S ** -0.5, 0.5, (), jnp.float32),
        "scalars": jnp.clip(jax.random.uniform(key_list[20], (SSMALL,), jnp.float32, 0.5, 1.0), 0.5, 1.0),
        "moment_narrowing": bell_draw(key_list[21], (D_S, B_S), (0.000055 * NALL ** -0.5), 4.172325134277344e-07, (), jnp.float32),
        "moment_attention": bell_draw(key_list[22], (B_S, 3 * B_S), (0.000055 * NALL ** -0.5), 4.172325134277344e-07, (), jnp.float32),
        "moment_combining": bell_draw(key_list[23], (B_S, B_S), (0.000055 * NALL ** -0.5), 4.172325134277344e-07, (), jnp.float32),
        "moment_expanding": bell_draw(key_list[24], (NFFN, B_S, FF_S), (0.000055 * NALL ** -0.5), 4.172325134277344e-07, (), jnp.float32),
        "moment_reducing": bell_draw(key_list[25], (NFFN, FF_S, B_S), (0.000055 * NALL ** -0.5), 4.172325134277344e-07, (), jnp.float32),
        "moment_widening": bell_draw(key_list[26], (B_S, D_S), (0.000055 * NALL ** -0.5), 4.172325134277344e-07, (), jnp.float32),
        "moment_scalars": bell_draw(key_list[27], (SSMALL,), (0.00022 * NALL ** -0.5), 1.6689300537109375e-06, (), jnp.float32),
        "square_narrowing": jnp.clip(jnp.exp(jax.random.uniform(key_list[28], (D_S, B_S), jnp.float32, math.log(1.7193001971473884e-16), math.log(2.7508803154358214e-15))), 1.7193001971473884e-16, 2.7508803154358214e-15),
        "square_attention": jnp.clip(jnp.exp(jax.random.uniform(key_list[29], (B_S, 3 * B_S), jnp.float32, math.log(1.7193001971473884e-16), math.log(2.7508803154358214e-15))), 1.7193001971473884e-16, 2.7508803154358214e-15),
        "square_combining": jnp.clip(jnp.exp(jax.random.uniform(key_list[30], (B_S, B_S), jnp.float32, math.log(1.7193001971473884e-16), math.log(2.7508803154358214e-15))), 1.7193001971473884e-16, 2.7508803154358214e-15),
        "square_expanding": jnp.clip(jnp.exp(jax.random.uniform(key_list[31], (NFFN, B_S, FF_S), jnp.float32, math.log(1.7193001971473884e-16), math.log(2.7508803154358214e-15))), 1.7193001971473884e-16, 2.7508803154358214e-15),
        "square_reducing": jnp.clip(jnp.exp(jax.random.uniform(key_list[32], (NFFN, FF_S, B_S), jnp.float32, math.log(1.7193001971473884e-16), math.log(2.7508803154358214e-15))), 1.7193001971473884e-16, 2.7508803154358214e-15),
        "square_widening": jnp.clip(jnp.exp(jax.random.uniform(key_list[33], (B_S, D_S), jnp.float32, math.log(1.7193001971473884e-16), math.log(2.7508803154358214e-15))), 1.7193001971473884e-16, 2.7508803154358214e-15),
        "square_scalars": jnp.clip(jnp.exp(jax.random.uniform(key_list[34], (SSMALL,), jnp.float32, math.log(2.7508803154358214e-15), math.log(4.401408504697314e-14))), 2.7508803154358214e-15, 4.401408504697314e-14),
    }


NEG = -1000000000.0
EPS_NORM = 1e-06
CLIP = 0.0005
LRATE = 0.05
BETA_ONE = 0.9
BETA_TWO = 0.999
ADAM_EPS = 1e-08
DECAY = 0.01

@jax.custom_vjp
def low(v):
    return lax.optimization_barrier(v.astype(jnp.bfloat16)).astype(jnp.float32)

@jax.custom_vjp
def low_back(v):
    return v

def low_keep(v):
    return (low(v), None)

def low_pass(kept, grad):
    return (grad,)

def back_keep(v):
    return (v, None)

def back_low(kept, grad):
    return (low(grad),)
low.defvjp(low_keep, low_pass)
low_back.defvjp(back_keep, back_low)

def pieces(vector, widths):
    result = []
    start = 0
    for width in widths:
        result.append(vector[start:start + width])
        start += width
    return result

def teacher_parts(vector):
    return pieces(vector, [D_T] * 8 + [FF_T] + [D_T] * 3 + [D_S] * 3)

def student_parts(vector):
    return pieces(vector, [B_S] * 8 + [NFFN * FF_S] + [NFFN * B_S] * 3 + [D_S] * 3)

def product(left, right):
    return jnp.dot(left, right, precision=lax.Precision.HIGHEST, preferred_element_type=jnp.float32)

def layer_norm(values, gain, shift):
    centred = values - lax.optimization_barrier(jnp.mean(values, -1, keepdims=True))
    spread = lax.optimization_barrier(jnp.mean(centred * centred, -1, keepdims=True))
    return centred * lax.rsqrt(spread + EPS_NORM) * gain + shift

def identity(values):
    return values

def head_scores(queries, keys, size, valid, wrap):
    raw = jnp.einsum('qhd,khd->hqk', queries.reshape(queries.shape[0], -1, size), keys.reshape(keys.shape[0], -1, size), precision=lax.Precision.HIGHEST) / math.sqrt(size)
    return jnp.where(valid[None, None, :], wrap(raw), NEG)

def head_mix(probs, values, size):
    mixed = jnp.einsum('hqk,khd->qhd', probs, values.reshape(values.shape[0], -1, size), precision=lax.Precision.HIGHEST)
    return mixed.reshape(mixed.shape[0], -1)

def embed(token_row, ends, frozen, embed_scalars):
    word_table, trigram_conv, position_table, segment_table = frozen
    rows = word_table[token_row]
    border = jnp.zeros((1, rows.shape[1]), jnp.float32)
    trigram = jnp.concatenate([jnp.concatenate([rows[1:], border], 0), rows, jnp.concatenate([border, rows[:-1]], 0)], -1)
    second = (jnp.arange(LEN, dtype=jnp.int32) >= ends[0]).astype(jnp.float32)[:, None]
    summed = product(trigram, trigram_conv) + position_table + segment_table[0] * (1.0 - second) + segment_table[1] * second
    return low(summed * embed_scalars[0] + embed_scalars[1])

def teacher(inputs, valid, weights):
    enter_weight, attend_weight, combine_weight, expand_weight, shrink_weight, leave_weight, teacher_scalars = weights
    piece = teacher_parts(teacher_scalars)
    front = layer_norm(product(inputs, enter_weight) + piece[0], piece[1], piece[2])
    blank = jnp.zeros((D_T,), jnp.float32)
    packed = low(product(low(front), attend_weight) + jnp.concatenate([piece[3], blank, piece[4]]))
    scores = head_scores(packed[:, :D_T], packed[:, D_T:2 * D_T], HD_T, valid, identity)
    logs = jax.nn.log_softmax(scores, -1)
    mixed = low(head_mix(low(jnp.exp(logs)), packed[:, 2 * D_T:], HD_T))
    hidden = layer_norm(product(mixed, combine_weight) + piece[5] + front, piece[6], piece[7])
    expanded = low(jax.nn.gelu(product(low(hidden), expand_weight) + piece[8], approximate=False))
    hidden = layer_norm(product(expanded, shrink_weight) + piece[9] + hidden, piece[10], piece[11])
    target = layer_norm(product(low(hidden), leave_weight) + piece[12] + inputs, piece[13], piece[14])
    return (target, logs)

def student(params, inputs, valid, target, teacher_logs):
    narrowing, attention, combining, expanding, reducing, widening, scalars = params
    piece = student_parts(scalars)
    live = valid.astype(jnp.float32)
    narrow_out = low_back(product(inputs, low(narrowing)) + piece[0]) * piece[1] + piece[2]
    blank = jnp.zeros((B_S,), jnp.float32)
    packed = low(low_back(product(low(narrow_out), low(attention)) + jnp.concatenate([piece[3], blank, piece[4]])))
    scores = head_scores(packed[:, :B_S], packed[:, B_S:2 * B_S], HD_S, valid, low_back)
    logs = jax.nn.log_softmax(scores, -1)
    mixed = low(low_back(head_mix(low(jnp.exp(logs)), packed[:, 2 * B_S:], HD_S)))
    hidden = (low_back(product(mixed, low(combining)) + piece[5]) + narrow_out) * piece[6] + piece[7]
    up_bias = piece[8].reshape(NFFN, FF_S)
    down_bias = piece[9].reshape(NFFN, B_S)
    feed_gain = piece[10].reshape(NFFN, B_S)
    feed_shift = piece[11].reshape(NFFN, B_S)
    for layer in range(NFFN):
        pre = low_back(product(low(hidden), low(expanding[layer])) + up_bias[layer])
        branch = low_back(product(low(jnp.maximum(pre, 0.0)), low(reducing[layer])) + down_bias[layer])
        hidden = (hidden + branch) * feed_gain[layer] + feed_shift[layer]
    output = (low_back(product(low(hidden), low(widening)) + piece[12]) + inputs) * piece[13] + piece[14]
    feature = jnp.sum(live * lax.optimization_barrier(jnp.mean((output - target) ** 2, -1)))
    transfer = jnp.sum(live[None, :, None] * jnp.where(valid[None, None, :], jnp.exp(teacher_logs) * (teacher_logs - logs), 0.0)) / HEADS
    return feature + transfer

def row_loss(params, token_row, ends, frozen, embed_scalars, teacher_weights):
    inputs = embed(token_row, ends, frozen, embed_scalars)
    valid = jnp.arange(LEN, dtype=jnp.int32) < ends[1]
    target, teacher_logs = teacher(inputs, valid, teacher_weights)
    return student(params, inputs, valid, target, teacher_logs)

def adam_update(weight, moment, square, grad, decay, stepf):
    first = BETA_ONE * moment + (1.0 - BETA_ONE) * grad
    second = BETA_TWO * square + (1.0 - BETA_TWO) * grad * grad
    first_hat = first / (1.0 - jnp.power(BETA_ONE, stepf))
    second_hat = second / (1.0 - jnp.power(BETA_TWO, stepf))
    return (weight - LRATE * (first_hat / (jnp.sqrt(second_hat) + ADAM_EPS) + decay * weight), first, second)

def reference(tokens, segment_ends, word_table, trigram_conv, position_table, segment_table, embed_scalars, teacher_enter, teacher_attention, teacher_combine, teacher_expand, teacher_reduce, teacher_leave, teacher_scalars, narrowing, attention, combining, expanding, reducing, widening, scalars, moment_narrowing, moment_attention, moment_combining, moment_expanding, moment_reducing, moment_widening, moment_scalars, square_narrowing, square_attention, square_combining, square_expanding, square_reducing, square_widening, square_scalars):
    frozen = tuple((w.astype(jnp.float32) for w in (word_table, trigram_conv, position_table, segment_table)))
    teacher_weights = tuple((w.astype(jnp.float32) for w in (teacher_enter, teacher_attention, teacher_combine, teacher_expand, teacher_reduce, teacher_leave))) + (teacher_scalars,)
    params = (narrowing, attention, combining, expanding, reducing, widening, scalars)
    count = jnp.sum(segment_ends[:, :, 1].astype(jnp.float32))
    flat_tokens = tokens.reshape(MB * ROWS, LEN)
    flat_ends = segment_ends.reshape(MB * ROWS, 2)

    def total(params):

        def one_row(carry, row):
            return (carry + jax.checkpoint(row_loss)(params, row[0], row[1], frozen, embed_scalars, teacher_weights), None)
        summed, unused = lax.scan(one_row, jnp.zeros((), jnp.float32), (flat_tokens, flat_ends))
        return summed / count
    loss, pullback = jax.vjp(total, params)
    grads = pullback(jnp.ones((), jnp.float32))[0]
    grad_norm = jnp.sqrt(sum((jnp.sum(g * g) for g in grads)))
    factor = CLIP / jnp.maximum(grad_norm, CLIP)
    stepf = jnp.asarray(STEP, jnp.float32)
    moments = (moment_narrowing, moment_attention, moment_combining, moment_expanding, moment_reducing, moment_widening, moment_scalars)
    squares = (square_narrowing, square_attention, square_combining, square_expanding, square_reducing, square_widening, square_scalars)
    results = [adam_update(params[index], moments[index], squares[index], grads[index] * factor, DECAY if index < 6 else 0.0, stepf) for index in range(7)]
    return (results[0][0], results[1][0], results[2][0], results[3][0], results[4][0], results[5][0], results[6][0], results[0][1], results[1][1], results[2][1], results[3][1], results[4][1], results[5][1], results[6][1], results[0][2], results[1][2], results[2][2], results[3][2], results[4][2], results[5][2], results[6][2], loss.reshape(1), grad_norm.reshape(1))
```

```python
import functools
import math

import jax
import jax.numpy as jnp
from jax import lax
from jax.experimental import pallas as pl
from jax.experimental.pallas import tpu as pltpu
from jax.sharding import PartitionSpec as P

D_S = 512
B_S = 128
HEADS = 4
FF_S = 512
NFFN = 4
D_T = 1024
FF_T = 4096
MB = 2
STEP = 10
HD_S = 32
HD_T = 256

NEG = -1000000000.0
EPS_NORM = 1e-06
CLIP = 0.0005
LRATE = 0.05
BETA_ONE = 0.9
BETA_TWO = 0.999
ADAM_EPS = 1e-08
DECAY = 0.01

LOG2E = math.log2(math.e)
LN2 = math.log(2.0)
SCALE_T = LOG2E / math.sqrt(HD_T)
SCALE_S = LOG2E / math.sqrt(HD_S)
NEG_T = NEG * LOG2E / SCALE_T
NEG_S = NEG * LOG2E / SCALE_S
KEY_SCALE = 1.0 / math.sqrt(HD_S)

F32 = jnp.float32
BF16 = jnp.bfloat16
BLOCK = 256
HALF = 128
VMEM_BYTES = 62 * 1024 * 1024

NN = (((1,), (0,)), ((), ()))
NT = (((1,), (1,)), ((), ()))
TN = (((0,), (0,)), ((), ()))


def dot(a, b, dims=NN):
    return lax.dot_general(a, b, dims, preferred_element_type=F32)


def params(**more):
    return pltpu.CompilerParams(vmem_limit_bytes=VMEM_BYTES, **more)


def whole(shape):
    zeros = (0,) * len(shape)
    return pl.BlockSpec(shape, lambda i, *s: zeros, pipeline_mode=pl.Buffered(1))


def at(i, meta):
    return jnp.minimum(i, meta[2] - 1)


def rows(width, block=BLOCK):
    return pl.BlockSpec((block, width), lambda i, meta, *s: (at(i, meta), 0))


def when_live(body):
    def run(meta, *refs):
        pl.when(pl.program_id(0) < meta[2])(functools.partial(body, meta, *refs))

    return run


def norm(values, gain, shift):
    centred = values - jnp.mean(values, -1, keepdims=True)
    spread = jnp.mean(centred * centred, -1, keepdims=True)
    return centred * lax.rsqrt(spread + EPS_NORM) * gain + shift


T_WIDTHS = [D_T] * 8 + [FF_T] + [D_T] * 3 + [D_S] * 3
S_WIDTHS = [B_S] * 8 + [NFFN * FF_S] + [NFFN * B_S] * 3 + [D_S] * 3


def tpart(ref, n):
    start = sum(T_WIDTHS[:n])
    return ref[0:1, start : start + T_WIDTHS[n]]


def spart(ref, n, layer=None):
    start, width = sum(S_WIDTHS[:n]), S_WIDTHS[n]
    if layer is not None:
        width = width // NFFN
        start += layer * width
    return ref[0:1, start : start + width]


def seg(meta, row):
    return meta[3 + 3 * row], meta[4 + 3 * row], meta[5 + 3 * row]


def live_slots(meta, nr, first, shape, axis):
    slot = first + lax.broadcasted_iota(jnp.int32, shape, axis)
    core = meta[0]
    live = slot < 0
    for row in range(nr):
        base, half, length = seg(meta, row)
        spot = core * half + slot - base
        inside = (slot >= base) & (slot < base + half)
        live = live | (inside & (spot < length))
    return live


def peers_of(n_dp, n_seq):
    dp, seq = lax.axis_index("dp"), lax.axis_index("seq")
    return dp, seq, dp * n_seq + seq


def share_body(n_dp, n_seq, mine, all_o, send_sem, recv_sem, own_sem):
    dp, seq, me = peers_of(n_dp, n_seq)
    total = n_dp * n_seq

    def device(step):
        other = lax.rem(me + step, total)
        return {"dp": lax.div(other, n_seq), "seq": lax.rem(other, n_seq)}

    barrier = pltpu.get_barrier_semaphore()

    @pl.loop(1, total)
    def _(step):
        pl.semaphore_signal(barrier, inc=1, device_id=device(step), device_id_type=pl.DeviceIdType.MESH)

    pl.semaphore_wait(barrier, total - 1)

    def copy(step):
        return pltpu.make_async_remote_copy(
            src_ref=mine,
            dst_ref=all_o.at[me],
            send_sem=send_sem.at[step],
            recv_sem=recv_sem.at[step],
            device_id=device(step),
            device_id_type=pl.DeviceIdType.MESH,
        )

    local = pltpu.make_async_copy(mine, all_o.at[me], own_sem)
    local.start()

    @pl.loop(1, total)
    def _(step):
        copy(step).start()

    local.wait()

    @pl.loop(1, total)
    def _(step):
        copy(step).wait()


def share(n_dp, n_seq, mine):
    total = n_dp * n_seq
    return pl.pallas_call(
        functools.partial(share_body, n_dp, n_seq),
        in_specs=[pl.BlockSpec(memory_space=pltpu.VMEM)],
        out_specs=pl.BlockSpec(memory_space=pltpu.VMEM),
        out_shape=jax.ShapeDtypeStruct((total,) + mine.shape, mine.dtype),
        scratch_shapes=[
            pltpu.SemaphoreType.DMA((total,)),
            pltpu.SemaphoreType.DMA((total,)),
            pltpu.SemaphoreType.DMA,
        ],
        compiler_params=params(collective_id=0, has_side_effects=True),
        name="share",
    )(mine)


def pick_seg(meta, nr, slot):
    base, half, length = seg(meta, 0)
    second = meta[3 + 3 * nr]
    for row in range(1, nr):
        nbase, nhalf, nlength = seg(meta, row)
        use = slot >= nbase
        base, half = jnp.where(use, nbase, base), jnp.where(use, nhalf, half)
        second = jnp.where(use, meta[3 + 3 * nr + row], second)
    return base, half, second


def embed_body(nr, cap, full, meta, words, places, conv, segments, scalars, inputs_o):
    step = pl.program_id(0)
    start = pl.multiple_of(step * BLOCK, BLOCK)
    core = meta[0]
    here = words[pl.ds(start, BLOCK), :].astype(F32)
    past = pl.multiple_of(jnp.maximum(start - 16, 0), 16)
    ahead = pl.multiple_of(start + BLOCK, 16)
    before = jnp.concatenate([words[pl.ds(past, 16), :].astype(F32)[15:16], here[:-1]], 0)
    after = jnp.concatenate([here[1:], words[pl.ds(ahead, 16), :].astype(F32)[0:1]], 0)
    slot = start + lax.broadcasted_iota(jnp.int32, (BLOCK, 1), 0)
    edge = words[cap : cap + 16, :].astype(F32)
    for row in range(nr):
        base, half, length = seg(meta, row)
        left = jnp.where(core > 0, edge[2 * row : 2 * row + 1], 0.0)
        right = jnp.where((core + 1) * half < full, edge[2 * row + 1 : 2 * row + 2], 0.0)
        before = jnp.where(slot == base, left, before)
        after = jnp.where(slot == base + half - 1, right, after)
    trigram = jnp.concatenate([after, here, before], 1).astype(BF16)
    summed = dot(trigram, conv[...])
    local = places.shape[1]
    for side in range(2):
        first = start + side * HALF
        base, half, border = pick_seg(meta, nr, first)
        spot = jnp.minimum(core * half + first - base, full - HALF)
        piece = jnp.bitwise_xor(lax.div(spot, local), meta[3 + 4 * nr])
        rest = pl.multiple_of(lax.rem(spot, local), HALF)
        place = places[piece, pl.ds(rest, HALF), :].astype(F32)
        second = (spot + lax.broadcasted_iota(jnp.int32, (HALF, 1), 0) >= border).astype(F32)
        part = (
            summed[side * HALF : (side + 1) * HALF]
            + place
            + segments[0:1].astype(F32) * (1.0 - second)
            + segments[1:2].astype(F32) * second
        )
        inputs_o[side * HALF : (side + 1) * HALF, :] = (part * scalars[0:1] + scalars[1:2]).astype(BF16)


def embed(nr, full, meta, words, places, conv, segments, scalars):
    cap = nr * full // 2
    ins = (words, places, conv, segments, scalars)
    return pl.pallas_call(
        when_live(functools.partial(embed_body, nr, cap, full)),
        grid_spec=pltpu.PrefetchScalarGridSpec(
            num_scalar_prefetch=1,
            grid=(cap // BLOCK,),
            in_specs=[whole(a.shape) for a in ins],
            out_specs=rows(D_S),
        ),
        out_shape=jax.ShapeDtypeStruct((cap, D_S), BF16),
        compiler_params=params(),
        name="embed",
    )(meta, *ins)


def project_body(own, meta, x, enter, wq, wk, wv, tsc, narrow, sattn, ssc, *refs):
    wvt, vcol, skt_w, svt_w, scol = refs[-5:]
    if own:
        front_o, q_o, k_o, vt_o, npre_o, nbf_o, sq_o, sk_o, skt_o, sv_o, svt_o = refs[:-5]
    else:
        k_o, vt_o, sk_o, skt_o, sv_o, svt_o = refs[6:-5]

    @pl.when(pl.program_id(0) == 0)
    def _():
        wvt[...] = wv[...].T
        vcol[...] = jnp.broadcast_to(tpart(tsc, 4), (HALF, D_T)).T
        skt_w[...] = sattn[:, B_S : 2 * B_S].T.astype(BF16)
        svt_w[...] = sattn[:, 2 * B_S :].T.astype(BF16)
        scol[...] = jnp.broadcast_to(spart(ssc, 4), (HALF, B_S)).T

    inputs = x[...]
    front = norm(dot(inputs, enter[...]) + tpart(tsc, 0), tpart(tsc, 1), tpart(tsc, 2))
    low = front.astype(BF16)
    if own:
        front_o[...] = front
        q_o[...] = (dot(low, wq[...]) + tpart(tsc, 3)).astype(BF16)
    k_o[...] = dot(low, wk[...]).astype(BF16).reshape(2, 1, HALF, D_T)
    vt = (dot(wvt[...], low, NT) + vcol[:, 0:1]).astype(BF16)
    vt_o[0] = vt[:, :HALF]
    vt_o[1] = vt[:, HALF:]
    npre = dot(inputs, narrow[...].astype(BF16)) + spart(ssc, 0)
    nbf = (npre * spart(ssc, 1) + spart(ssc, 2)).astype(BF16)
    packed = dot(nbf, sattn[...].astype(BF16))
    if own:
        npre_o[...] = npre
        nbf_o[...] = nbf
        sq_o[...] = (packed[:, :B_S] + spart(ssc, 3)).astype(BF16)
    sk_o[...] = packed[:, B_S : 2 * B_S].astype(BF16).reshape(2, 1, HALF, B_S)
    sv_o[...] = (packed[:, 2 * B_S :] + spart(ssc, 4)).astype(BF16).reshape(2, 1, HALF, B_S)
    skt = dot(skt_w[...], nbf, NT).astype(BF16)
    skt_o[0] = skt[:, :HALF]
    skt_o[1] = skt[:, HALF:]
    svt = (dot(svt_w[...], nbf, NT) + scol[:, 0:1]).astype(BF16)
    svt_o[0] = svt[:, :HALF]
    svt_o[1] = svt[:, HALF:]


def project(own, meta, x, weights, kept=()):
    cap = x.shape[0]
    nblk = cap // HALF
    side = 0 if own else 1
    key_shape = lambda w: jax.ShapeDtypeStruct((nblk, 2, HALF, w), BF16)
    flip_shape = lambda w: jax.ShapeDtypeStruct((nblk, w, 2 * HALF), BF16)
    key_spec = lambda w: pl.BlockSpec((2, 1, HALF, w), lambda i, meta, *s: (at(i, meta), side, 0, 0))
    flip_spec = lambda w: pl.BlockSpec((2, w, HALF), lambda i, meta, *s: (at(i, meta), 0, side))
    tok = lambda w, t: jax.ShapeDtypeStruct((cap, w), t)
    shared = [(key_shape(D_T), key_spec(D_T)), (flip_shape(D_T), flip_spec(D_T))]
    small = [
        (key_shape(B_S), key_spec(B_S)),
        (flip_shape(B_S), flip_spec(B_S)),
        (key_shape(B_S), key_spec(B_S)),
        (flip_shape(B_S), flip_spec(B_S)),
    ]
    enter, packed, tsc, narrow, sattn, ssc = weights
    third = lambda n: pl.BlockSpec((D_T, D_T), lambda i, *s: (0, n), pipeline_mode=pl.Buffered(1))
    ins = [
        (x, rows(D_S)), (enter, whole(enter.shape)), (packed, third(0 if own else 1)), (packed, third(1)), (packed, third(2)),
        (tsc, whole(tsc.shape)), (narrow, whole(narrow.shape)), (sattn, whole(sattn.shape)), (ssc, whole(ssc.shape)),
    ]
    if own:
        outs = [(tok(D_T, F32), rows(D_T)), (tok(D_T, BF16), rows(D_T))] + shared
        outs += [(tok(B_S, F32), rows(B_S)), (tok(B_S, BF16), rows(B_S)), (tok(B_S, BF16), rows(B_S))] + small
        alias = {}
    else:
        outs = shared + small
        alias = {1 + len(ins) + n: n for n in range(6)}
    return pl.pallas_call(
        when_live(functools.partial(project_body, own)),
        grid_spec=pltpu.PrefetchScalarGridSpec(
            num_scalar_prefetch=1,
            grid=(cap // BLOCK,),
            in_specs=[spec for _, spec in ins] + [pl.BlockSpec(memory_space=pl.ANY)] * len(kept),
            out_specs=[spec for _, spec in outs],
            scratch_shapes=[
                pltpu.VMEM((D_T, D_T), BF16),
                pltpu.VMEM((D_T, HALF), F32),
                pltpu.VMEM((B_S, B_S), BF16),
                pltpu.VMEM((B_S, B_S), BF16),
                pltpu.VMEM((B_S, HALF), F32),
            ],
        ),
        out_shape=[shape for shape, _ in outs],
        input_output_aliases=alias,
        compiler_params=params(),
        name="project_own" if own else "project_peer",
    )(meta, *[a for a, _ in ins], *kept)


def dead_keys(meta, row, chunk):
    base, half, length = seg(meta, row)
    spot = lax.broadcasted_iota(jnp.int32, (2 * HALF, BLOCK), 0)
    mine = meta[0] * half + chunk * HALF + spot
    other = (1 - meta[0]) * half + chunk * HALF + spot - HALF
    return jnp.where(spot < HALF, mine, other) >= length


def head_masked(values, head):
    lane = lax.broadcasted_iota(jnp.int32, values.shape, 1)
    return jnp.where((lane >= head * HD_S) & (lane < (head + 1) * HD_S), values, jnp.zeros_like(values))


def chunk_loops(meta, row, body, carry):
    base, half, length = seg(meta, row)
    count = lax.div(half, HALF)
    full = jnp.clip(lax.div(length - half, HALF), 0, count)
    carry = lax.fori_loop(0, full, functools.partial(body, False), carry)
    return lax.fori_loop(full, count, functools.partial(body, True), carry)


def attend_body(nr, meta, q, k, vt, sq, sk, svt, mixed_o, smixed_o, lse_o, e_scr, m_scr, acc_t, acc_s):
    consts = [SCALE_T] * HEADS + [SCALE_S] * HEADS
    for row in range(nr):
        base, half, length = seg(meta, row)
        first = lax.div(base, HALF)

        def one_block(step, unused, row=row, base=base, first=first):
            start = pl.multiple_of(base + step * BLOCK, HALF)
            q_all = q[pl.ds(start, BLOCK), :]
            s_all = sq[pl.ds(start, BLOCK), :]
            heads_s = [head_masked(s_all, h) for h in range(HEADS)]

            def scores(masked, chunk, carry):
                spot = first + chunk
                dead = dead_keys(meta, row, chunk) if masked else None
                result = []
                for n in range(2 * HEADS):
                    h = n % HEADS
                    if n < HEADS:
                        raw = dot(k[spot, :, h * HD_T : (h + 1) * HD_T], q_all[:, h * HD_T : (h + 1) * HD_T], NT)
                    else:
                        raw = dot(sk[spot], heads_s[h], NT)
                    if masked:
                        raw = jnp.where(dead, NEG_T if n < HEADS else NEG_S, raw)
                    top, total = carry[n]
                    split = raw.reshape(2 * HALF // 8, 8, BLOCK)
                    new = jnp.maximum(top, jnp.max(split, 0))
                    e = jnp.exp2((split - new) * consts[n])
                    e_scr[chunk, n] = e.reshape(2 * HALF, BLOCK)
                    m_scr[chunk, n] = new
                    total = total * jnp.exp2((top - new) * consts[n]) + jnp.sum(e, 0)
                    result.append((new, total))
                return tuple(result)

            start_stat = (jnp.full((8, BLOCK), -3e38, F32), jnp.zeros((8, BLOCK), F32))
            stats = chunk_loops(meta, row, scores, tuple([start_stat] * (2 * HEADS)))
            tops, scales = [], []
            lines = []
            for n in range(2 * HEADS):
                top, total = stats[n]
                best = jnp.max(top, 0, keepdims=True)
                summed = jnp.sum(total * jnp.exp2((top - best) * consts[n]), 0, keepdims=True)
                tops.append(best)
                scales.append(1.0 / summed)
                lines.append(best * consts[n] + jnp.log2(summed))
            lse = jnp.concatenate(lines, 0)
            lse_o[lax.div(start, HALF)] = lse[:, :HALF]
            lse_o[lax.div(start, HALF) + 1] = lse[:, HALF:]
            acc_t[...] = jnp.zeros_like(acc_t)
            acc_s[...] = jnp.zeros_like(acc_s)

            def mix(chunk, unused):
                spot = first + chunk
                for n in range(2 * HEADS):
                    h = n % HEADS
                    factor = jnp.exp2((m_scr[chunk, n] - tops[n]) * consts[n]) * scales[n]
                    e = e_scr[chunk, n].reshape(2 * HALF // 8, 8, BLOCK)
                    p = (e * factor).reshape(2 * HALF, BLOCK).astype(BF16)
                    if n < HEADS:
                        acc_t[h] += dot(vt[spot, h * HD_T : (h + 1) * HD_T, :], p)
                    else:
                        acc_s[h] += dot(svt[spot, h * HD_S : (h + 1) * HD_S, :], p)
                return unused

            lax.fori_loop(0, lax.div(meta[4 + 3 * row], HALF), mix, 0)
            for h in range(HEADS):
                mixed_o[pl.ds(start, BLOCK), h * HD_T : (h + 1) * HD_T] = acc_t[h].T.astype(BF16)
            smixed_o[pl.ds(start, BLOCK), :] = acc_s[...].reshape(B_S, BLOCK).T
            return unused

        lax.fori_loop(0, lax.div(half + BLOCK - 1, BLOCK), one_block, 0)


def attend(nr, meta, q, k, vt, sq, sk, svt):
    cap = q.shape[0]
    nblk = cap // HALF
    chunks = 8
    ins = (q, k, vt, sq, sk, svt)
    outs = [
        jax.ShapeDtypeStruct((cap, D_T), BF16),
        jax.ShapeDtypeStruct((cap, B_S), F32),
        jax.ShapeDtypeStruct((nblk, 8, HALF), F32),
    ]
    return pl.pallas_call(
        functools.partial(attend_body, nr),
        grid_spec=pltpu.PrefetchScalarGridSpec(
            num_scalar_prefetch=1,
            grid=(1,),
            in_specs=[whole(a.shape) for a in ins],
            out_specs=[whole(a.shape) for a in outs],
            scratch_shapes=[
                pltpu.VMEM((chunks, 2 * HEADS, 2 * HALF, BLOCK), F32),
                pltpu.VMEM((chunks, 2 * HEADS, 8, BLOCK), F32),
                pltpu.VMEM((HEADS, HD_T, BLOCK), F32),
                pltpu.VMEM((HEADS, HD_S, BLOCK), F32),
            ],
        ),
        out_shape=outs,
        compiler_params=params(),
        name="attend",
    )(meta, *ins)


def teacher_body(meta, mixed, front, inputs, combine, expand, reduce, leave, tsc, target_o):
    hidden = norm(dot(mixed[...], combine[...]) + tpart(tsc, 5) + front[...], tpart(tsc, 6), tpart(tsc, 7))
    low = hidden.astype(BF16)
    total = jnp.zeros(hidden.shape, F32)
    width = 512
    bias = tpart(tsc, 8)
    for part in range(FF_T // width):
        cols = slice(part * width, (part + 1) * width)
        pre = dot(low, expand[:, cols]) + bias[:, cols]
        act = (0.5 * pre * (1.0 + lax.erf(pre * math.sqrt(0.5)))).astype(BF16)
        total = total + dot(act, reduce[cols, :])
    hidden = norm(total + tpart(tsc, 9) + hidden, tpart(tsc, 10), tpart(tsc, 11))
    last = dot(hidden.astype(BF16), leave[...]) + tpart(tsc, 12) + inputs[...].astype(F32)
    target_o[...] = norm(last, tpart(tsc, 13), tpart(tsc, 14))


def teacher_tail(meta, mixed, front, inputs, weights):
    cap = mixed.shape[0]
    return pl.pallas_call(
        when_live(teacher_body),
        grid_spec=pltpu.PrefetchScalarGridSpec(
            num_scalar_prefetch=1,
            grid=(cap // BLOCK,),
            in_specs=[rows(D_T), rows(D_T), rows(D_S)] + [whole(w.shape) for w in weights],
            out_specs=rows(D_S),
        ),
        out_shape=jax.ShapeDtypeStruct((cap, D_S), F32),
        compiler_params=params(),
        name="teacher_tail",
    )(meta, mixed, front, inputs, *weights)


def fold(values):
    return jnp.sum(values.reshape(values.shape[0] // 8, 8, values.shape[1]), 0)


def student_body(
    nr, meta, scale, smixed, npre, inputs, target, combine, expand, reduce, widen, ssc,
    dmix_o, datt_o, delta_o, early_o, gcomb_o, s128_o, s512_o, expand_w, reduce_w,
):
    step = pl.program_id(0)
    start = step * BLOCK
    live = live_slots(meta, nr, start, (BLOCK, 1), 0)

    @pl.when(step == 0)
    def _():
        for ref in (early_o, gcomb_o, s128_o, s512_o):
            ref[...] = jnp.zeros_like(ref)
        expand_w[...] = expand[...].astype(BF16)
        reduce_w[...] = reduce[...].astype(BF16)

    inside = start + lax.broadcasted_iota(jnp.int32, (BLOCK, 1), 0) < meta[1]
    mix = jnp.where(inside, smixed[...], 0.0)
    mix_low = mix.astype(BF16)
    combine_low = combine[...].astype(BF16)
    widen_low = widen[...].astype(BF16)
    narrow_out = npre[...] * spart(ssc, 1) + spart(ssc, 2)
    attend_sum = dot(mix_low, combine_low) + spart(ssc, 5) + narrow_out
    hidden = attend_sum * spart(ssc, 6) + spart(ssc, 7)
    layer_in, layer_on, layer_relu, layer_sums = [], [], [], []
    for n in range(NFFN):
        low = hidden.astype(BF16)
        pre = dot(low, expand_w[n]) + spart(ssc, 8, n)
        relu = jnp.maximum(pre, 0.0).astype(BF16)
        total = hidden + (dot(relu, reduce_w[n]) + spart(ssc, 9, n))
        layer_in.append(low)
        layer_on.append(pre > 0)
        layer_relu.append(relu)
        layer_sums.append(total)
        hidden = total * spart(ssc, 10, n) + spart(ssc, 11, n)
    last = hidden.astype(BF16)
    wide_sum = dot(last, widen_low) + spart(ssc, 12) + inputs[...].astype(F32)
    output = wide_sum * spart(ssc, 13) + spart(ssc, 14)
    gap = jnp.where(live, output - target[...], 0.0)
    d_out = gap * 2.0 / D_S * scale[0]
    s512_o[0] += fold(gap * gap)
    s512_o[1] += fold(d_out * wide_sum)
    s512_o[2] += fold(d_out)
    d_wide = (d_out * spart(ssc, 13)).astype(BF16)
    s512_o[3] += fold(d_wide.astype(F32))
    early_o[2 * NFFN * B_S :, :] += dot(last, d_wide, TN)
    d_hidden = dot(d_wide, widen_low, NT)
    for n in reversed(range(NFFN)):
        s128_o[n] += fold(d_hidden * layer_sums[n])
        s128_o[4 + n] += fold(d_hidden)
        d_sum = d_hidden * spart(ssc, 10, n)
        d_red = d_sum.astype(BF16)
        s128_o[8 + n] += fold(d_red.astype(F32))
        early_o[(NFFN + n) * B_S : (NFFN + n + 1) * B_S, :] += dot(d_red, layer_relu[n], TN)
        d_pre = jnp.where(layer_on[n], dot(d_red, reduce_w[n], NT), 0.0).astype(BF16)
        s512_o[4 + n] += fold(d_pre.astype(F32))
        early_o[n * B_S : (n + 1) * B_S, :] += dot(layer_in[n], d_pre, TN)
        d_hidden = d_sum + dot(d_pre, expand_w[n], NT)
    s128_o[12] += fold(d_hidden * attend_sum)
    s128_o[13] += fold(d_hidden)
    d_att = d_hidden * spart(ssc, 6)
    d_comb = d_att.astype(BF16)
    s128_o[14] += fold(d_comb.astype(F32))
    gcomb_o[...] += dot(mix_low, d_comb, TN)
    d_mix = dot(d_comb, combine_low, NT).astype(BF16)
    dmix_o[...] = d_mix
    datt_o[...] = d_att
    delta_o[...] = d_mix.astype(F32) * mix


EARLY = (2 * NFFN + 1) * B_S
LATE = 3 * B_S


def student_tail(nr, meta, scale, smixed, npre, inputs, target, weights):
    cap = smixed.shape[0]
    shape = lambda *s: jax.ShapeDtypeStruct(s, F32)
    sums = [shape(EARLY, D_S), shape(B_S, B_S), shape(15, 8, B_S), shape(8, 8, D_S)]
    return pl.pallas_call(
        when_live(functools.partial(student_body, nr)),
        grid_spec=pltpu.PrefetchScalarGridSpec(
            num_scalar_prefetch=2,
            grid=(cap // BLOCK,),
            in_specs=[rows(B_S), rows(B_S), rows(D_S), rows(D_S)] + [whole(w.shape) for w in weights],
            out_specs=[rows(B_S), rows(B_S), rows(B_S)] + [whole(s.shape) for s in sums],
            scratch_shapes=[pltpu.VMEM((NFFN, B_S, FF_S), BF16), pltpu.VMEM((NFFN, FF_S, B_S), BF16)],
        ),
        out_shape=[jax.ShapeDtypeStruct((cap, B_S), BF16), shape(cap, B_S), shape(cap, B_S)] + sums,
        compiler_params=params(),
        name="student_tail",
    )(meta, scale, smixed, npre, inputs, target, *weights)


def back_body(nr, meta, scale, q, k, sq, sk, skt, sv, dmix, delta, lse, dq_o, dk_o, dv_o, kl_o, acc_q):
    kl_o[...] = jnp.zeros_like(kl_o)
    for row in range(nr):
        base, half, length = seg(meta, row)
        first = lax.div(base, HALF)

        def clear(chunk, unused, first=first):
            dk_o[first + chunk] = jnp.zeros((2 * HALF, B_S), F32)
            dv_o[first + chunk] = jnp.zeros((2 * HALF, B_S), F32)
            return unused

        lax.fori_loop(0, lax.div(half, HALF), clear, 0)

        def one_block(step, unused, row=row, base=base, first=first, half=half, length=length):
            start = pl.multiple_of(base + step * BLOCK, HALF)
            inside = step * BLOCK + lax.broadcasted_iota(jnp.int32, (BLOCK, 1), 0) < half
            q_all = jnp.where(inside, q[pl.ds(start, BLOCK), :], jnp.zeros((), BF16))
            s_all = jnp.where(inside, sq[pl.ds(start, BLOCK), :], jnp.zeros((), BF16))
            m_all = jnp.where(inside, dmix[pl.ds(start, BLOCK), :], jnp.zeros((), BF16))
            flat = jnp.where(inside, delta[pl.ds(start, BLOCK), :], 0.0).T
            spot_q = step * BLOCK + lax.broadcasted_iota(jnp.int32, (1, BLOCK), 1)
            inside_q = spot_q < half
            live = inside_q & (meta[0] * half + spot_q < length)
            heads_s = [head_masked(s_all, h) for h in range(HEADS)]
            heads_m = [head_masked(m_all, h) for h in range(HEADS)]
            lines = jnp.concatenate([lse[lax.div(start, HALF)], lse[lax.div(start, HALF) + 1]], 1)
            lines = jnp.where(inside_q, lines, 1e9)
            weight = jnp.where(live, scale[1], 0.0)
            offsets = [weight - jnp.sum(flat[h * HD_S : (h + 1) * HD_S], 0, keepdims=True) for h in range(HEADS)]
            acc_q[...] = jnp.zeros_like(acc_q)
            stack_s = jnp.concatenate(heads_s, 0)
            stack_m = jnp.concatenate(heads_m, 0)

            def chunk_body(masked, chunk, kl):
                spot = first + chunk
                dead = dead_keys(meta, row, chunk) if masked else None
                probs, grads = [], []
                for h in range(HEADS):
                    z_t = dot(k[spot, :, h * HD_T : (h + 1) * HD_T], q_all[:, h * HD_T : (h + 1) * HD_T], NT) * SCALE_T
                    z_s = dot(sk[spot], heads_s[h], NT) * SCALE_S
                    d_p = dot(sv[spot], heads_m[h], NT)
                    if masked:
                        z_t = jnp.where(dead, NEG, z_t)
                        z_s = jnp.where(dead, NEG, z_s)
                    p_t = jnp.exp2(z_t - lines[h : h + 1])
                    p_s = jnp.exp2(z_s - lines[HEADS + h : HEADS + h + 1])
                    kl = kl + fold(p_t * (z_t - z_s)) * jnp.where(live, 1.0, 0.0)
                    d_s = p_s * (d_p + offsets[h]) - p_t * weight
                    probs.append(p_s.astype(BF16))
                    low = d_s.astype(BF16)
                    grads.append(low)
                    acc_q[h] += dot(skt[spot, h * HD_S : (h + 1) * HD_S, :], low)
                dv_o[spot] += dot(jnp.concatenate(probs, 1), stack_m)
                dk_o[spot] += dot(jnp.concatenate(grads, 1), stack_s)
                return kl

            kl = chunk_loops(meta, row, chunk_body, jnp.zeros((8, BLOCK), F32))
            rest = jnp.zeros((1, BLOCK), F32)
            for h in range(HEADS):
                rest = rest + lines[HEADS + h : HEADS + h + 1] - lines[h : h + 1]
            kl_o[0] += kl
            kl_o[1, 0:1] += jnp.where(live, rest, 0.0)
            dq_o[pl.ds(start, BLOCK), :] = acc_q[...].reshape(B_S, BLOCK).T
            return unused

        lax.fori_loop(0, lax.div(half + BLOCK - 1, BLOCK), one_block, 0)


def attend_back(nr, meta, scale, *ins):
    cap = ins[0].shape[0]
    nblk = cap // HALF
    outs = [
        jax.ShapeDtypeStruct((cap, B_S), F32),
        jax.ShapeDtypeStruct((nblk, 2 * HALF, B_S), F32),
        jax.ShapeDtypeStruct((nblk, 2 * HALF, B_S), F32),
        jax.ShapeDtypeStruct((2, 8, BLOCK), F32),
    ]
    return pl.pallas_call(
        functools.partial(back_body, nr),
        grid_spec=pltpu.PrefetchScalarGridSpec(
            num_scalar_prefetch=2,
            grid=(1,),
            in_specs=[whole(a.shape) for a in ins],
            out_specs=[whole(a.shape) for a in outs],
            scratch_shapes=[pltpu.VMEM((HEADS, HD_S, BLOCK), F32)],
        ),
        out_shape=outs,
        compiler_params=params(),
        name="attend_back",
    )(meta, scale, *ins)


def finish_body(
    meta, scale, dq, dk, dv, pk, pv, datt, npre, nbf, inputs, attention, ssc, gcomb, s128, s512, kl, late_o, t128, t384
):
    step = pl.program_id(0)

    @pl.when(step == 0)
    def _():
        for ref in (late_o, t128, t384):
            ref[...] = jnp.zeros_like(ref)

    inside = step * BLOCK + lax.broadcasted_iota(jnp.int32, (BLOCK, 1), 0) < meta[1]
    d_q = dq[...] * KEY_SCALE
    d_k = (dk[...].reshape(BLOCK, B_S) + pk[...].reshape(BLOCK, B_S).astype(F32)) * KEY_SCALE
    d_v = dv[...].reshape(BLOCK, B_S) + pv[...].reshape(BLOCK, B_S).astype(F32)
    d_all = jnp.where(inside, jnp.concatenate([d_q, d_k, d_v], 1), 0.0).astype(BF16)
    t384[...] += fold(d_all.astype(F32))
    late_o[B_S : 2 * B_S, B_S:] += dot(nbf[...], d_all, TN)
    d_narrow = datt[...] + dot(d_all, attention[...].astype(BF16), NT)
    t128[0] += fold(d_narrow * npre[...])
    t128[1] += fold(d_narrow)
    d_enter = (d_narrow * spart(ssc, 1)).astype(BF16)
    t128[2] += fold(d_enter.astype(F32))
    late_o[:B_S, :] += dot(d_enter, inputs[...], TN)

    @pl.when(step == meta[2] - 1)
    def _():
        line = lambda v: jnp.sum(v, 0, keepdims=True)
        join = lambda items: jnp.concatenate([line(v) for v in items], 1)
        late_o[B_S : 2 * B_S, :B_S] = gcomb[...]
        loss = jnp.sum(line(s512[0]), 1, keepdims=True) / D_S + (LN2 / HEADS) * (
            jnp.sum(line(kl[0]), 1, keepdims=True) + jnp.sum(line(kl[1]), 1, keepdims=True)
        )
        items = [
            join([t128[2], t128[0], t128[1], t384[:, :B_S]]),
            join([t384[:, 2 * B_S :], s128[14], s128[12], s128[13]]),
        ]
        items += [line(s512[4 + n]) for n in range(NFFN)]
        items += [join([s128[8 + n] for n in range(NFFN)]), join([s128[n] for n in range(NFFN)])]
        items += [join([s128[4 + n] for n in range(NFFN)]), line(s512[3]), line(s512[1]), line(s512[2])]
        items += [jnp.broadcast_to(loss * scale[0], (1, D_S)), jnp.zeros((3, D_S), F32)]
        late_o[2 * B_S : 2 * B_S + 16, :] = jnp.concatenate(items, 0)


def finish(meta, scale, dq, dk, dv, pk, pv, datt, npre, nbf, inputs, attention, ssc, gcomb, s128, s512, kl):
    cap = dq.shape[0]
    mine = pl.BlockSpec((2, 1, HALF, B_S), lambda i, meta, *s: (at(i, meta), 0, 0, 0))
    peer = pl.BlockSpec((2, HALF, B_S), lambda i, meta, *s: (at(i, meta), 0, 0))
    fixed = (attention, ssc, gcomb, s128, s512, kl)
    return pl.pallas_call(
        when_live(finish_body),
        grid_spec=pltpu.PrefetchScalarGridSpec(
            num_scalar_prefetch=2,
            grid=(cap // BLOCK,),
            in_specs=[rows(B_S), mine, mine, peer, peer, rows(B_S), rows(B_S), rows(B_S), rows(D_S)]
            + [whole(a.shape) for a in fixed],
            out_specs=whole((LATE, D_S)),
            scratch_shapes=[pltpu.VMEM((3, 8, B_S), F32), pltpu.VMEM((8, 3 * B_S), F32)],
        ),
        out_shape=jax.ShapeDtypeStruct((LATE, D_S), F32),
        compiler_params=params(),
        name="finish",
    )(meta, scale, dq, dk, dv, pk, pv, datt, npre, nbf, inputs, *fixed)


class Line:
    def __init__(self, size, spot, device):
        self.size, self.spot, self.device = size, spot, device


def lines_of(n_dp, n_seq):
    dp, seq = lax.axis_index("dp"), lax.axis_index("seq")
    n_low = line_sizes(n_dp, n_seq)[2]
    low, high = lax.rem(dp, n_low), lax.div(dp, n_low)
    core, y = lax.rem(seq, 2), lax.div(seq, 2)
    return (
        Line(2, core, lambda j: {"dp": dp, "seq": y * 2 + j}),
        Line(n_seq // 2, y, lambda j: {"dp": dp, "seq": j * 2 + core}),
        Line(n_low, low, lambda j: {"dp": high * n_low + j, "seq": seq}),
        Line(n_dp // n_low, high, lambda j: {"dp": j * n_low + low, "seq": seq}),
    )


def line_sizes(n_dp, n_seq):
    n_low = 2 if n_dp == 8 else 4
    return (2, n_seq // 2, n_low, n_dp // n_low)


def sum_plan(n_dp, n_seq, total):
    sizes = line_sizes(n_dp, n_seq)
    orders = ((0, 1, 2, 3), (0, 2, 1, 3))
    stages = []
    for level in range(4):
        stage = []
        for part, order in enumerate(orders):
            length = total // 2
            for done in order[:level]:
                length //= sizes[done]
            stage.append((part, order[level], length // sizes[order[level]]))
        stages.append(stage)
    return stages


def sum_body(n_dp, n_seq, total, early, late, out, *scratch):
    stages = sum_plan(n_dp, n_seq, total)
    buffers, work, send_sem, recv_sem = scratch[:-3], scratch[-3], scratch[-2], scratch[-1]
    lines = lines_of(n_dp, n_seq)
    sizes = line_sizes(n_dp, n_seq)

    barrier = pltpu.get_barrier_semaphore()
    met = 0
    for line, size in zip(lines, sizes, strict=True):
        for step in range(1, size):
            pl.semaphore_signal(
                barrier, inc=1, device_id=line.device(lax.rem(line.spot + step, size)), device_id_type=pl.DeviceIdType.MESH
            )
            met += 1
    work[: early.shape[0], :] = early[...]
    work[early.shape[0] : early.shape[0] + late.shape[0], :] = late[...]
    if total > early.shape[0] + late.shape[0]:
        work[early.shape[0] + late.shape[0] :, :] = jnp.zeros((total - early.shape[0] - late.shape[0], D_S), F32)
    pl.semaphore_wait(barrier, met)

    number = [0]

    def remote(src, dst, line, step, size):
        n = number[0]
        number[0] += 1
        copy = pltpu.make_async_remote_copy(
            src_ref=src, dst_ref=dst, send_sem=send_sem.at[n], recv_sem=recv_sem.at[n],
            device_id=line.device(lax.rem(line.spot + step, size)), device_id_type=pl.DeviceIdType.MESH,
        )
        copy.start()
        return copy

    region = [0, total // 2]
    trail = []
    slot = 0
    for stage in stages:
        copies = []
        for part, axis, sub in stage:
            line, size = lines[axis], sizes[axis]
            buffer = buffers[slot]
            slot += 1
            for step in range(1, size):
                target = lax.rem(line.spot + step, size)
                start = pl.multiple_of(region[part] + target * sub, 8)
                copies.append(remote(work.at[pl.ds(start, sub), :], buffer.at[step - 1], line, step, size))
        for copy in copies:
            copy.wait()
        slot -= len(stage)
        level = []
        for part, axis, sub in stage:
            line, size = lines[axis], sizes[axis]
            start = pl.multiple_of(region[part] + line.spot * sub, 8)
            value = work[pl.ds(start, sub), :]
            for step in range(1, size):
                value = value + buffers[slot][step - 1]
            slot += 1
            (out if stage is stages[-1] else work)[pl.ds(start, sub), :] = value
            region[part] = start
            level.append((line, size, sub, start))
        trail.append(level)
    for level in reversed(trail):
        copies = []
        for line, size, sub, start in level:
            piece = out.at[pl.ds(start, sub), :]
            for step in range(1, size):
                copies.append(remote(piece, piece, line, step, size))
        for copy in copies:
            copy.wait()


def sum_all(n_dp, n_seq, early, late):
    sizes = line_sizes(n_dp, n_seq)
    unit = 2 * 8
    for size in sizes:
        unit *= size
    total = -(-(early.shape[0] + late.shape[0]) // unit) * unit
    stages = sum_plan(n_dp, n_seq, total)
    buffers = [pltpu.VMEM((sizes[axis] - 1, sub, D_S), F32) for stage in stages for _, axis, sub in stage]
    count = 2 * 2 * sum(size - 1 for size in sizes)
    return pl.pallas_call(
        functools.partial(sum_body, n_dp, n_seq, total),
        in_specs=[pl.BlockSpec(memory_space=pltpu.VMEM)] * 2,
        out_specs=pl.BlockSpec(memory_space=pltpu.VMEM),
        out_shape=jax.ShapeDtypeStruct((total, D_S), F32),
        scratch_shapes=buffers + [pltpu.VMEM((total, D_S), F32), pltpu.SemaphoreType.DMA((count,)), pltpu.SemaphoreType.DMA((count,))],
        compiler_params=params(collective_id=1, has_side_effects=True),
        name="sum_all",
    )(early, late)


FIRST_FIX = 1.0 / (1.0 - BETA_ONE**STEP)
SECOND_FIX = 1.0 / (1.0 - BETA_TWO**STEP)


def adam_body(grads, *refs):
    weights, moments, squares = refs[:7], refs[7:14], refs[14:21]
    new_w, new_m, new_s, norm_o = refs[21:28], refs[28:35], refs[35:42], refs[42]
    top = EARLY + 2 * B_S
    total = jnp.zeros((8, D_S), F32)
    for start in range(0, top, B_S):
        part = grads[start : start + B_S, :]
        total = total + fold(part * part)
    extra = grads[top : top + 12, :]
    square = jnp.sum(total, 0, keepdims=True) + jnp.sum(extra * extra, 0, keepdims=True)
    grad_norm = jnp.sqrt(jnp.sum(square, 1, keepdims=True))
    norm_o[0:1, :] = jnp.broadcast_to(grad_norm, (1, HALF))
    norm_o[1:2, :] = grads[top + 12 : top + 13, :HALF]
    factor = CLIP / jnp.maximum(grad_norm, CLIP)

    def update(n, where, grad):
        g = grad * factor
        weight = weights[n][where]
        first = BETA_ONE * moments[n][where] + (1.0 - BETA_ONE) * g
        second = BETA_TWO * squares[n][where] + (1.0 - BETA_TWO) * g * g
        change = (first * FIRST_FIX) / (jnp.sqrt(second * SECOND_FIX) + ADAM_EPS)
        if n < 6:
            change = change + DECAY * weight
        new_w[n][where] = weight - LRATE * change
        new_m[n][where] = first
        new_s[n][where] = second

    every = (slice(None), slice(None))
    update(0, every, grads[EARLY : EARLY + B_S, :].T)
    update(1, every, grads[EARLY + B_S : top, B_S:])
    update(2, every, grads[EARLY + B_S : top, :B_S])
    for n in range(NFFN):
        update(3, n, grads[n * B_S : (n + 1) * B_S, :])
        update(4, n, grads[(NFFN + n) * B_S : (NFFN + n + 1) * B_S, :].T)
    update(5, every, grads[2 * NFFN * B_S : EARLY, :])
    for n in range(12):
        update(6, (slice(0, 1), slice(n * D_S, (n + 1) * D_S)), grads[top + n : top + n + 1, :])


def adam(grads, weights, moments, squares):
    like = [jax.ShapeDtypeStruct(w.shape, F32) for w in weights]
    outs = like * 3 + [jax.ShapeDtypeStruct((2, HALF), F32)]
    return pl.pallas_call(
        adam_body,
        in_specs=[pl.BlockSpec(memory_space=pltpu.VMEM)] * 22,
        out_specs=[pl.BlockSpec(memory_space=pltpu.VMEM)] * 22,
        out_shape=outs,
        compiler_params=params(),
        name="adam",
    )(grads, *weights, *moments, *squares)


def shards(
    tokens, segment_ends, word_table, trigram_conv, position_table, segment_table, embed_scalars,
    teacher_enter, teacher_attention, teacher_combine, teacher_expand, teacher_reduce, teacher_leave, teacher_scalars,
    narrowing, attention, combining, expanding, reducing, widening, scalars, *state,
):
    micros, rows_here, local = tokens.shape
    n_dp, n_seq = lax.axis_size("dp"), lax.axis_size("seq")
    full = local * n_seq
    half_cap = full // 2
    n_rows = micros * rows_here * n_dp
    n_chips = n_dp * n_seq // 2
    nr = n_rows // n_chips
    cap = nr * half_cap
    seq = lax.axis_index("seq")
    core = seq % 2
    chip = lax.axis_index("dp") * (n_seq // 2) + seq // 2
    swap = [(i, i ^ 1) for i in range(n_seq)]

    token_lines = micros * rows_here * local // HALF
    ends_line = jnp.pad(segment_ends.reshape(1, -1), ((0, 0), (0, HALF - micros * rows_here * 2)))
    told = share(n_dp, n_seq, jnp.concatenate([tokens.reshape(token_lines, HALF), ends_line], 0))
    if n_seq == 4:
        side = lax.ppermute(position_table, "seq", swap)
        cross = lax.ppermute(position_table, "seq", [(i, i ^ 2) for i in range(4)])
        corner = lax.ppermute(cross, "seq", swap)
        places = jnp.stack([position_table, side, cross, corner])
        turn = seq
    else:
        places = lax.all_gather(position_table, "seq", axis=0)
        turn = jnp.int32(0)

    ends = told[:, token_lines, : micros * rows_here * 2].reshape(n_dp, n_seq, micros * rows_here, 2)[:, 0]
    ends = ends.reshape(n_rows, 2)
    lengths = ends[:, 1]
    count = jnp.sum(lengths.astype(F32))
    order = jnp.arange(n_rows, dtype=jnp.int32)
    ahead = (lengths[None, :] > lengths[:, None]) | (
        (lengths[None, :] == lengths[:, None]) & (order[None, :] < order[:, None])
    )
    rank = jnp.sum(ahead.astype(jnp.int32), 1)
    picks = []
    for j in range(nr):
        wanted = j * n_chips + (chip if j % 2 == 0 else n_chips - 1 - chip)
        hit = (rank == wanted).astype(jnp.int32)
        picks.append((jnp.sum(hit * order), jnp.sum(hit * ends[:, 0]), jnp.sum(hit * lengths)))
    halves = [(length + 255) // 256 * HALF for _, _, length in picks]
    bases = [sum(halves[:j], jnp.int32(0)) for j in range(nr)]
    slots = sum(halves, jnp.int32(0))
    meta = [core, slots, (slots + BLOCK - 1) // BLOCK]
    for j in range(nr):
        meta += [bases[j], halves[j], picks[j][2]]
    meta += [pick[1] for pick in picks] + [turn]
    meta = jnp.stack([jnp.asarray(v, jnp.int32) for v in meta])
    scale_back = 1.0 / count
    scale = jnp.stack([scale_back, scale_back / HEADS])

    ids = jnp.zeros((cap,), jnp.int32)
    edges = []
    every = told[:, :token_lines].reshape(n_dp, n_seq, micros * rows_here, local)
    for j in range(nr):
        owner, inner = picks[j][0] // (micros * rows_here), picks[j][0] % (micros * rows_here)
        line = lax.dynamic_slice(every, (owner, 0, inner, 0), (1, n_seq, 1, local)).reshape(full)
        first = core * halves[j]
        edges += [
            lax.dynamic_slice(line, (jnp.maximum(first - 1, 0),), (1,)),
            lax.dynamic_slice(line, (jnp.minimum(first + halves[j], full - 1),), (1,)),
        ]
        ids = lax.dynamic_update_slice(ids, lax.dynamic_slice(line, (first,), (half_cap,)), (bases[j],))
    ids = jnp.concatenate([ids] + edges + [jnp.zeros((16 - 2 * nr,), jnp.int32)])
    words = word_table.at[ids].get(mode="promise_in_bounds")
    inputs = embed(nr, full, meta, words, places, trigram_conv, segment_table, embed_scalars)
    peer_inputs = lax.ppermute(inputs, "seq", swap)

    tsc = teacher_scalars.reshape(1, -1)
    ssc = scalars.reshape(1, -1)
    weights = (teacher_enter, teacher_attention, tsc, narrowing, attention, ssc)
    front, q, k, vt, npre, nbf, sq, sk, skt, sv, svt = project(True, meta, inputs, weights)
    k, vt, sk, skt, sv, svt = project(False, meta, peer_inputs, weights, (k, vt, sk, skt, sv, svt))
    nblk = k.shape[0]
    k3 = k.reshape(nblk, 2 * HALF, D_T)
    sk3 = sk.reshape(nblk, 2 * HALF, B_S)
    sv3 = sv.reshape(nblk, 2 * HALF, B_S)
    mixed, smixed, lse = attend(nr, meta, q, k3, vt, sq, sk3, svt)
    target = teacher_tail(
        meta, mixed, front, inputs, (teacher_combine, teacher_expand, teacher_reduce, teacher_leave, tsc)
    )
    dmix, datt, delta, early, g_comb, s128, s512 = student_tail(
        nr, meta, scale, smixed, npre, inputs, target, (combining, expanding, reducing, widening, ssc)
    )
    dq, dk, dv, kl = attend_back(nr, meta, scale, q, k3, sq, sk3, skt, sv3, dmix, delta, lse)
    dk = dk.reshape(nblk, 2, HALF, B_S)
    dv = dv.reshape(nblk, 2, HALF, B_S)
    pk = lax.ppermute(dk[:, 1].astype(BF16), "seq", swap)
    pv = lax.ppermute(dv[:, 1].astype(BF16), "seq", swap)
    late = finish(meta, scale, dq, dk, dv, pk, pv, datt, npre, nbf, inputs, attention, ssc, g_comb, s128, s512, kl)
    grads = sum_all(n_dp, n_seq, early, late)
    flat = lambda items: list(items[:6]) + [items[6].reshape(1, -1)]
    outs = adam(
        grads,
        [narrowing, attention, combining, expanding, reducing, widening, ssc],
        flat(state[:7]),
        flat(state[7:14]),
    )
    final = []
    for n in range(3):
        final += list(outs[7 * n : 7 * n + 6]) + [outs[7 * n + 6].reshape(-1)]
    return tuple(final) + (outs[21][1, :1], outs[21][0, :1])


def solution(mesh):
    specs = [P()] * 35
    specs[0] = P(None, "dp", "seq")
    specs[1] = P(None, "dp", None)
    specs[4] = P("seq", None)
    return jax.shard_map(
        shards, mesh=mesh, in_specs=tuple(specs), out_specs=tuple([P()] * 23), check_vma=False
    )
```

```python
import functools
import math

import jax
import jax.numpy as jnp
from jax import lax
from jax.experimental import pallas as pl
from jax.experimental.pallas import tpu as pltpu
from jax.sharding import PartitionSpec as P

D_S = 512
B_S = 128
HEADS = 4
FF_S = 512
NFFN = 4
D_T = 1024
FF_T = 4096
MB = 2
STEP = 10
HD_S = 32
HD_T = 256

NEG = -1000000000.0
EPS_NORM = 1e-06
CLIP = 0.0005
LRATE = 0.05
BETA_ONE = 0.9
BETA_TWO = 0.999
ADAM_EPS = 1e-08
DECAY = 0.01

LOG2E = math.log2(math.e)
LN2 = math.log(2.0)
SCALE_T = LOG2E / math.sqrt(HD_T)
SCALE_S = LOG2E / math.sqrt(HD_S)
NEG_T = NEG * LOG2E / SCALE_T
NEG_S = NEG * LOG2E / SCALE_S
KEY_SCALE = 1.0 / math.sqrt(HD_S)

F32 = jnp.float32
BF16 = jnp.bfloat16
BLOCK = 256
HALF = 128
VMEM_BYTES = 62 * 1024 * 1024

NN = (((1,), (0,)), ((), ()))
NT = (((1,), (1,)), ((), ()))
TN = (((0,), (0,)), ((), ()))


def dot(a, b, dims=NN):
    return lax.dot_general(a, b, dims, preferred_element_type=F32)


def params(**more):
    return pltpu.CompilerParams(vmem_limit_bytes=VMEM_BYTES, **more)


def whole(shape):
    zeros = (0,) * len(shape)
    return pl.BlockSpec(shape, lambda i, *s: zeros, pipeline_mode=pl.Buffered(1))


def at(i, meta):
    return jnp.minimum(i, meta[2] - 1)


def rows(width, block=BLOCK):
    return pl.BlockSpec((block, width), lambda i, meta, *s: (at(i, meta), 0))


def when_live(body):
    def run(meta, *refs):
        pl.when(pl.program_id(0) < meta[2])(functools.partial(body, meta, *refs))

    return run


def norm(values, gain, shift):
    centred = values - jnp.mean(values, -1, keepdims=True)
    spread = jnp.mean(centred * centred, -1, keepdims=True)
    return centred * lax.rsqrt(spread + EPS_NORM) * gain + shift


T_WIDTHS = [D_T] * 8 + [FF_T] + [D_T] * 3 + [D_S] * 3
S_WIDTHS = [B_S] * 8 + [NFFN * FF_S] + [NFFN * B_S] * 3 + [D_S] * 3


def tpart(ref, n):
    start = sum(T_WIDTHS[:n])
    return ref[0:1, start : start + T_WIDTHS[n]]


def spart(ref, n, layer=None):
    start, width = sum(S_WIDTHS[:n]), S_WIDTHS[n]
    if layer is not None:
        width = width // NFFN
        start += layer * width
    return ref[0:1, start : start + width]


def seg(meta, row):
    return meta[3 + 3 * row], meta[4 + 3 * row], meta[5 + 3 * row]


def live_slots(meta, nr, first, shape, axis):
    slot = first + lax.broadcasted_iota(jnp.int32, shape, axis)
    core = meta[0]
    live = slot < 0
    for row in range(nr):
        base, half, length = seg(meta, row)
        spot = core * half + slot - base
        inside = (slot >= base) & (slot < base + half)
        live = live | (inside & (spot < length))
    return live


def peers_of(n_dp, n_seq):
    dp, seq = lax.axis_index("dp"), lax.axis_index("seq")
    return dp, seq, dp * n_seq + seq


def share_body(n_dp, n_seq, mine, all_o, send_sem, recv_sem, own_sem):
    dp, seq, me = peers_of(n_dp, n_seq)
    total = n_dp * n_seq

    def device(step):
        other = lax.rem(me + step, total)
        return {"dp": lax.div(other, n_seq), "seq": lax.rem(other, n_seq)}

    barrier = pltpu.get_barrier_semaphore()

    @pl.loop(1, total)
    def _(step):
        pl.semaphore_signal(barrier, inc=1, device_id=device(step), device_id_type=pl.DeviceIdType.MESH)

    pl.semaphore_wait(barrier, total - 1)

    def copy(step):
        return pltpu.make_async_remote_copy(
            src_ref=mine,
            dst_ref=all_o.at[me],
            send_sem=send_sem.at[step],
            recv_sem=recv_sem.at[step],
            device_id=device(step),
            device_id_type=pl.DeviceIdType.MESH,
        )

    local = pltpu.make_async_copy(mine, all_o.at[me], own_sem)
    local.start()

    @pl.loop(1, total)
    def _(step):
        copy(step).start()

    local.wait()

    @pl.loop(1, total)
    def _(step):
        copy(step).wait()


def share(n_dp, n_seq, mine):
    total = n_dp * n_seq
    return pl.pallas_call(
        functools.partial(share_body, n_dp, n_seq),
        in_specs=[pl.BlockSpec(memory_space=pltpu.VMEM)],
        out_specs=pl.BlockSpec(memory_space=pltpu.VMEM),
        out_shape=jax.ShapeDtypeStruct((total,) + mine.shape, mine.dtype),
        scratch_shapes=[
            pltpu.SemaphoreType.DMA((total,)),
            pltpu.SemaphoreType.DMA((total,)),
            pltpu.SemaphoreType.DMA,
        ],
        compiler_params=params(collective_id=0, has_side_effects=True),
        name="share",
    )(mine)


def pick_seg(meta, nr, slot):
    base, half, length = seg(meta, 0)
    second = meta[3 + 3 * nr]
    for row in range(1, nr):
        nbase, nhalf, nlength = seg(meta, row)
        use = slot >= nbase
        base, half = jnp.where(use, nbase, base), jnp.where(use, nhalf, half)
        second = jnp.where(use, meta[3 + 3 * nr + row], second)
    return base, half, second


def embed_body(nr, cap, full, meta, words, places, conv, segments, scalars, inputs_o):
    step = pl.program_id(0)
    start = pl.multiple_of(step * BLOCK, BLOCK)
    core = meta[0]
    here = words[pl.ds(start, BLOCK), :].astype(F32)
    past = pl.multiple_of(jnp.maximum(start - 16, 0), 16)
    ahead = pl.multiple_of(start + BLOCK, 16)
    before = jnp.concatenate([words[pl.ds(past, 16), :].astype(F32)[15:16], here[:-1]], 0)
    after = jnp.concatenate([here[1:], words[pl.ds(ahead, 16), :].astype(F32)[0:1]], 0)
    slot = start + lax.broadcasted_iota(jnp.int32, (BLOCK, 1), 0)
    edge = words[cap : cap + 16, :].astype(F32)
    for row in range(nr):
        base, half, length = seg(meta, row)
        left = jnp.where(core > 0, edge[2 * row : 2 * row + 1], 0.0)
        right = jnp.where((core + 1) * half < full, edge[2 * row + 1 : 2 * row + 2], 0.0)
        before = jnp.where(slot == base, left, before)
        after = jnp.where(slot == base + half - 1, right, after)
    trigram = jnp.concatenate([after, here, before], 1).astype(BF16)
    summed = dot(trigram, conv[...])
    local = places.shape[1]
    for side in range(2):
        first = start + side * HALF
        base, half, border = pick_seg(meta, nr, first)
        spot = jnp.minimum(core * half + first - base, full - HALF)
        piece = jnp.bitwise_xor(lax.div(spot, local), meta[3 + 4 * nr])
        rest = pl.multiple_of(lax.rem(spot, local), HALF)
        place = places[piece, pl.ds(rest, HALF), :].astype(F32)
        second = (spot + lax.broadcasted_iota(jnp.int32, (HALF, 1), 0) >= border).astype(F32)
        part = (
            summed[side * HALF : (side + 1) * HALF]
            + place
            + segments[0:1].astype(F32) * (1.0 - second)
            + segments[1:2].astype(F32) * second
        )
        inputs_o[side * HALF : (side + 1) * HALF, :] = (part * scalars[0:1] + scalars[1:2]).astype(BF16)


def embed(nr, full, meta, words, places, conv, segments, scalars):
    cap = nr * full // 2
    ins = (words, places, conv, segments, scalars)
    return pl.pallas_call(
        when_live(functools.partial(embed_body, nr, cap, full)),
        grid_spec=pltpu.PrefetchScalarGridSpec(
            num_scalar_prefetch=1,
            grid=(cap // BLOCK,),
            in_specs=[whole(a.shape) for a in ins],
            out_specs=rows(D_S),
        ),
        out_shape=jax.ShapeDtypeStruct((cap, D_S), BF16),
        compiler_params=params(),
        name="embed",
    )(meta, *ins)


def project_body(own, meta, x, enter, wq, wk, wv, tsc, narrow, sattn, ssc, *refs):
    wvt, vcol, skt_w, svt_w, scol = refs[-5:]
    if own:
        front_o, q_o, k_o, vt_o, npre_o, nbf_o, sq_o, sk_o, skt_o, sv_o, svt_o = refs[:-5]
    else:
        k_o, vt_o, sk_o, skt_o, sv_o, svt_o = refs[6:-5]

    @pl.when(pl.program_id(0) == 0)
    def _():
        wvt[...] = wv[...].T
        vcol[...] = jnp.broadcast_to(tpart(tsc, 4), (HALF, D_T)).T
        skt_w[...] = sattn[:, B_S : 2 * B_S].T.astype(BF16)
        svt_w[...] = sattn[:, 2 * B_S :].T.astype(BF16)
        scol[...] = jnp.broadcast_to(spart(ssc, 4), (HALF, B_S)).T

    inputs = x[...]
    front = norm(dot(inputs, enter[...]) + tpart(tsc, 0), tpart(tsc, 1), tpart(tsc, 2))
    low = front.astype(BF16)
    if own:
        front_o[...] = front
        q_o[...] = (dot(low, wq[...]) + tpart(tsc, 3)).astype(BF16)
    k_o[...] = dot(low, wk[...]).astype(BF16).reshape(2, 1, HALF, D_T)
    vt = (dot(wvt[...], low, NT) + vcol[:, 0:1]).astype(BF16)
    vt_o[0] = vt[:, :HALF]
    vt_o[1] = vt[:, HALF:]
    npre = dot(inputs, narrow[...].astype(BF16)) + spart(ssc, 0)
    nbf = (npre * spart(ssc, 1) + spart(ssc, 2)).astype(BF16)
    packed = dot(nbf, sattn[...].astype(BF16))
    if own:
        npre_o[...] = npre
        nbf_o[...] = nbf
        sq_o[...] = (packed[:, :B_S] + spart(ssc, 3)).astype(BF16)
    sk_o[...] = packed[:, B_S : 2 * B_S].astype(BF16).reshape(2, 1, HALF, B_S)
    sv_o[...] = (packed[:, 2 * B_S :] + spart(ssc, 4)).astype(BF16).reshape(2, 1, HALF, B_S)
    skt = dot(skt_w[...], nbf, NT).astype(BF16)
    skt_o[0] = skt[:, :HALF]
    skt_o[1] = skt[:, HALF:]
    svt = (dot(svt_w[...], nbf, NT) + scol[:, 0:1]).astype(BF16)
    svt_o[0] = svt[:, :HALF]
    svt_o[1] = svt[:, HALF:]


def project(own, meta, x, weights, kept=()):
    cap = x.shape[0]
    nblk = cap // HALF
    side = 0 if own else 1
    key_shape = lambda w: jax.ShapeDtypeStruct((nblk, 2, HALF, w), BF16)
    flip_shape = lambda w: jax.ShapeDtypeStruct((nblk, w, 2 * HALF), BF16)
    key_spec = lambda w: pl.BlockSpec((2, 1, HALF, w), lambda i, meta, *s: (at(i, meta), side, 0, 0))
    flip_spec = lambda w: pl.BlockSpec((2, w, HALF), lambda i, meta, *s: (at(i, meta), 0, side))
    tok = lambda w, t: jax.ShapeDtypeStruct((cap, w), t)
    shared = [(key_shape(D_T), key_spec(D_T)), (flip_shape(D_T), flip_spec(D_T))]
    small = [
        (key_shape(B_S), key_spec(B_S)),
        (flip_shape(B_S), flip_spec(B_S)),
        (key_shape(B_S), key_spec(B_S)),
        (flip_shape(B_S), flip_spec(B_S)),
    ]
    enter, packed, tsc, narrow, sattn, ssc = weights
    third = lambda n: pl.BlockSpec((D_T, D_T), lambda i, *s: (0, n), pipeline_mode=pl.Buffered(1))
    ins = [
        (x, rows(D_S)), (enter, whole(enter.shape)), (packed, third(0 if own else 1)), (packed, third(1)), (packed, third(2)),
        (tsc, whole(tsc.shape)), (narrow, whole(narrow.shape)), (sattn, whole(sattn.shape)), (ssc, whole(ssc.shape)),
    ]
    if own:
        outs = [(tok(D_T, F32), rows(D_T)), (tok(D_T, BF16), rows(D_T))] + shared
        outs += [(tok(B_S, F32), rows(B_S)), (tok(B_S, BF16), rows(B_S)), (tok(B_S, BF16), rows(B_S))] + small
        alias = {}
    else:
        outs = shared + small
        alias = {1 + len(ins) + n: n for n in range(6)}
    return pl.pallas_call(
        when_live(functools.partial(project_body, own)),
        grid_spec=pltpu.PrefetchScalarGridSpec(
            num_scalar_prefetch=1,
            grid=(cap // BLOCK,),
            in_specs=[spec for _, spec in ins] + [pl.BlockSpec(memory_space=pl.ANY)] * len(kept),
            out_specs=[spec for _, spec in outs],
            scratch_shapes=[
                pltpu.VMEM((D_T, D_T), BF16),
                pltpu.VMEM((D_T, HALF), F32),
                pltpu.VMEM((B_S, B_S), BF16),
                pltpu.VMEM((B_S, B_S), BF16),
                pltpu.VMEM((B_S, HALF), F32),
            ],
        ),
        out_shape=[shape for shape, _ in outs],
        input_output_aliases=alias,
        compiler_params=params(),
        name="project_own" if own else "project_peer",
    )(meta, *[a for a, _ in ins], *kept)


def dead_keys(meta, row, chunk):
    base, half, length = seg(meta, row)
    spot = lax.broadcasted_iota(jnp.int32, (2 * HALF, BLOCK), 0)
    mine = meta[0] * half + chunk * HALF + spot
    other = (1 - meta[0]) * half + chunk * HALF + spot - HALF
    return jnp.where(spot < HALF, mine, other) >= length


def head_masked(values, head):
    lane = lax.broadcasted_iota(jnp.int32, values.shape, 1)
    return jnp.where((lane >= head * HD_S) & (lane < (head + 1) * HD_S), values, jnp.zeros_like(values))


def chunk_loops(meta, row, body, carry):
    base, half, length = seg(meta, row)
    count = lax.div(half, HALF)
    full = jnp.clip(lax.div(length - half, HALF), 0, count)
    carry = lax.fori_loop(0, full, functools.partial(body, False), carry)
    return lax.fori_loop(full, count, functools.partial(body, True), carry)


def attend_body(nr, meta, q, k, vt, sq, sk, svt, mixed_o, smixed_o, lse_o, e_scr, m_scr, acc_t, acc_s):
    consts = [SCALE_T] * HEADS + [SCALE_S] * HEADS
    for row in range(nr):
        base, half, length = seg(meta, row)
        first = lax.div(base, HALF)

        def one_block(step, unused, row=row, base=base, first=first):
            start = pl.multiple_of(base + step * BLOCK, HALF)
            q_all = q[pl.ds(start, BLOCK), :]
            s_all = sq[pl.ds(start, BLOCK), :]
            heads_s = [head_masked(s_all, h) for h in range(HEADS)]

            def scores(masked, chunk, carry):
                spot = first + chunk
                dead = dead_keys(meta, row, chunk) if masked else None
                result = []
                for n in range(2 * HEADS):
                    h = n % HEADS
                    if n < HEADS:
                        raw = dot(k[spot, :, h * HD_T : (h + 1) * HD_T], q_all[:, h * HD_T : (h + 1) * HD_T], NT)
                    else:
                        raw = dot(sk[spot], heads_s[h], NT)
                    if masked:
                        raw = jnp.where(dead, NEG_T if n < HEADS else NEG_S, raw)
                    top, total = carry[n]
                    split = raw.reshape(2 * HALF // 8, 8, BLOCK)
                    new = jnp.maximum(top, jnp.max(split, 0))
                    e = jnp.exp2((split - new) * consts[n])
                    e_scr[chunk, n] = e.reshape(2 * HALF, BLOCK)
                    m_scr[chunk, n] = new
                    total = total * jnp.exp2((top - new) * consts[n]) + jnp.sum(e, 0)
                    result.append((new, total))
                return tuple(result)

            start_stat = (jnp.full((8, BLOCK), -3e38, F32), jnp.zeros((8, BLOCK), F32))
            stats = chunk_loops(meta, row, scores, tuple([start_stat] * (2 * HEADS)))
            tops, scales = [], []
            lines = []
            for n in range(2 * HEADS):
                top, total = stats[n]
                best = jnp.max(top, 0, keepdims=True)
                summed = jnp.sum(total * jnp.exp2((top - best) * consts[n]), 0, keepdims=True)
                tops.append(best)
                scales.append(1.0 / summed)
                lines.append(best * consts[n] + jnp.log2(summed))
            lse = jnp.concatenate(lines, 0)
            lse_o[lax.div(start, HALF)] = lse[:, :HALF]
            lse_o[lax.div(start, HALF) + 1] = lse[:, HALF:]
            acc_t[...] = jnp.zeros_like(acc_t)
            acc_s[...] = jnp.zeros_like(acc_s)

            def mix(chunk, unused):
                spot = first + chunk
                for n in range(2 * HEADS):
                    h = n % HEADS
                    factor = jnp.exp2((m_scr[chunk, n] - tops[n]) * consts[n]) * scales[n]
                    e = e_scr[chunk, n].reshape(2 * HALF // 8, 8, BLOCK)
                    p = (e * factor).reshape(2 * HALF, BLOCK).astype(BF16)
                    if n < HEADS:
                        acc_t[h] += dot(vt[spot, h * HD_T : (h + 1) * HD_T, :], p)
                    else:
                        acc_s[h] += dot(svt[spot, h * HD_S : (h + 1) * HD_S, :], p)
                return unused

            lax.fori_loop(0, lax.div(meta[4 + 3 * row], HALF), mix, 0)
            for h in range(HEADS):
                mixed_o[pl.ds(start, BLOCK), h * HD_T : (h + 1) * HD_T] = acc_t[h].T.astype(BF16)
            smixed_o[pl.ds(start, BLOCK), :] = acc_s[...].reshape(B_S, BLOCK).T
            return unused

        lax.fori_loop(0, lax.div(half + BLOCK - 1, BLOCK), one_block, 0)


def attend(nr, meta, q, k, vt, sq, sk, svt):
    cap = q.shape[0]
    nblk = cap // HALF
    chunks = 8
    ins = (q, k, vt, sq, sk, svt)
    outs = [
        jax.ShapeDtypeStruct((cap, D_T), BF16),
        jax.ShapeDtypeStruct((cap, B_S), F32),
        jax.ShapeDtypeStruct((nblk, 8, HALF), F32),
    ]
    return pl.pallas_call(
        functools.partial(attend_body, nr),
        grid_spec=pltpu.PrefetchScalarGridSpec(
            num_scalar_prefetch=1,
            grid=(1,),
            in_specs=[whole(a.shape) for a in ins],
            out_specs=[whole(a.shape) for a in outs],
            scratch_shapes=[
                pltpu.VMEM((chunks, 2 * HEADS, 2 * HALF, BLOCK), F32),
                pltpu.VMEM((chunks, 2 * HEADS, 8, BLOCK), F32),
                pltpu.VMEM((HEADS, HD_T, BLOCK), F32),
                pltpu.VMEM((HEADS, HD_S, BLOCK), F32),
            ],
        ),
        out_shape=outs,
        compiler_params=params(),
        name="attend",
    )(meta, *ins)


def teacher_body(meta, mixed, front, inputs, combine, expand, reduce, leave, tsc, target_o):
    hidden = norm(dot(mixed[...], combine[...]) + tpart(tsc, 5) + front[...], tpart(tsc, 6), tpart(tsc, 7))
    low = hidden.astype(BF16)
    total = jnp.zeros(hidden.shape, F32)
    width = 512
    bias = tpart(tsc, 8)
    for part in range(FF_T // width):
        cols = slice(part * width, (part + 1) * width)
        pre = dot(low, expand[:, cols]) + bias[:, cols]
        act = (0.5 * pre * (1.0 + lax.erf(pre * math.sqrt(0.5)))).astype(BF16)
        total = total + dot(act, reduce[cols, :])
    hidden = norm(total + tpart(tsc, 9) + hidden, tpart(tsc, 10), tpart(tsc, 11))
    last = dot(hidden.astype(BF16), leave[...]) + tpart(tsc, 12) + inputs[...].astype(F32)
    target_o[...] = norm(last, tpart(tsc, 13), tpart(tsc, 14))


def teacher_tail(meta, mixed, front, inputs, weights):
    cap = mixed.shape[0]
    return pl.pallas_call(
        when_live(teacher_body),
        grid_spec=pltpu.PrefetchScalarGridSpec(
            num_scalar_prefetch=1,
            grid=(cap // BLOCK,),
            in_specs=[rows(D_T), rows(D_T), rows(D_S)] + [whole(w.shape) for w in weights],
            out_specs=rows(D_S),
        ),
        out_shape=jax.ShapeDtypeStruct((cap, D_S), F32),
        compiler_params=params(),
        name="teacher_tail",
    )(meta, mixed, front, inputs, *weights)


def fold(values):
    return jnp.sum(values.reshape(values.shape[0] // 8, 8, values.shape[1]), 0)


def student_body(
    nr, meta, scale, smixed, npre, inputs, target, combine, expand, reduce, widen, ssc,
    dmix_o, datt_o, delta_o, early_o, gcomb_o, s128_o, s512_o, expand_w, reduce_w,
):
    step = pl.program_id(0)
    start = step * BLOCK
    live = live_slots(meta, nr, start, (BLOCK, 1), 0)

    @pl.when(step == 0)
    def _():
        for ref in (early_o, gcomb_o, s128_o, s512_o):
            ref[...] = jnp.zeros_like(ref)
        expand_w[...] = expand[...].astype(BF16)
        reduce_w[...] = reduce[...].astype(BF16)

    inside = start + lax.broadcasted_iota(jnp.int32, (BLOCK, 1), 0) < meta[1]
    mix = jnp.where(inside, smixed[...], 0.0)
    mix_low = mix.astype(BF16)
    combine_low = combine[...].astype(BF16)
    widen_low = widen[...].astype(BF16)
    narrow_out = npre[...] * spart(ssc, 1) + spart(ssc, 2)
    attend_sum = dot(mix_low, combine_low) + spart(ssc, 5) + narrow_out
    hidden = attend_sum * spart(ssc, 6) + spart(ssc, 7)
    layer_in, layer_on, layer_relu, layer_sums = [], [], [], []
    for n in range(NFFN):
        low = hidden.astype(BF16)
        pre = dot(low, expand_w[n]) + spart(ssc, 8, n)
        relu = jnp.maximum(pre, 0.0).astype(BF16)
        total = hidden + (dot(relu, reduce_w[n]) + spart(ssc, 9, n))
        layer_in.append(low)
        layer_on.append(pre > 0)
        layer_relu.append(relu)
        layer_sums.append(total)
        hidden = total * spart(ssc, 10, n) + spart(ssc, 11, n)
    last = hidden.astype(BF16)
    wide_sum = dot(last, widen_low) + spart(ssc, 12) + inputs[...].astype(F32)
    output = wide_sum * spart(ssc, 13) + spart(ssc, 14)
    gap = jnp.where(live, output - target[...], 0.0)
    d_out = gap * 2.0 / D_S * scale[0]
    s512_o[0] += fold(gap * gap)
    s512_o[1] += fold(d_out * wide_sum)
    s512_o[2] += fold(d_out)
    d_wide = (d_out * spart(ssc, 13)).astype(BF16)
    s512_o[3] += fold(d_wide.astype(F32))
    early_o[2 * NFFN * B_S :, :] += dot(last, d_wide, TN)
    d_hidden = dot(d_wide, widen_low, NT)
    for n in reversed(range(NFFN)):
        s128_o[n] += fold(d_hidden * layer_sums[n])
        s128_o[4 + n] += fold(d_hidden)
        d_sum = d_hidden * spart(ssc, 10, n)
        d_red = d_sum.astype(BF16)
        s128_o[8 + n] += fold(d_red.astype(F32))
        early_o[(NFFN + n) * B_S : (NFFN + n + 1) * B_S, :] += dot(d_red, layer_relu[n], TN)
        d_pre = jnp.where(layer_on[n], dot(d_red, reduce_w[n], NT), 0.0).astype(BF16)
        s512_o[4 + n] += fold(d_pre.astype(F32))
        early_o[n * B_S : (n + 1) * B_S, :] += dot(layer_in[n], d_pre, TN)
        d_hidden = d_sum + dot(d_pre, expand_w[n], NT)
    s128_o[12] += fold(d_hidden * attend_sum)
    s128_o[13] += fold(d_hidden)
    d_att = d_hidden * spart(ssc, 6)
    d_comb = d_att.astype(BF16)
    s128_o[14] += fold(d_comb.astype(F32))
    gcomb_o[...] += dot(mix_low, d_comb, TN)
    d_mix = dot(d_comb, combine_low, NT).astype(BF16)
    dmix_o[...] = d_mix
    datt_o[...] = d_att
    delta_o[...] = d_mix.astype(F32) * mix


EARLY = (2 * NFFN + 1) * B_S
LATE = 3 * B_S


def student_tail(nr, meta, scale, smixed, npre, inputs, target, weights):
    cap = smixed.shape[0]
    shape = lambda *s: jax.ShapeDtypeStruct(s, F32)
    sums = [shape(EARLY, D_S), shape(B_S, B_S), shape(15, 8, B_S), shape(8, 8, D_S)]
    return pl.pallas_call(
        when_live(functools.partial(student_body, nr)),
        grid_spec=pltpu.PrefetchScalarGridSpec(
            num_scalar_prefetch=2,
            grid=(cap // BLOCK,),
            in_specs=[rows(B_S), rows(B_S), rows(D_S), rows(D_S)] + [whole(w.shape) for w in weights],
            out_specs=[rows(B_S), rows(B_S), rows(B_S)] + [whole(s.shape) for s in sums],
            scratch_shapes=[pltpu.VMEM((NFFN, B_S, FF_S), BF16), pltpu.VMEM((NFFN, FF_S, B_S), BF16)],
        ),
        out_shape=[jax.ShapeDtypeStruct((cap, B_S), BF16), shape(cap, B_S), shape(cap, B_S)] + sums,
        compiler_params=params(),
        name="student_tail",
    )(meta, scale, smixed, npre, inputs, target, *weights)


def back_body(nr, meta, scale, q, k, sq, sk, skt, sv, dmix, delta, lse, dq_o, dk_o, dv_o, kl_o, acc_q, p_scr, g_scr, s_scr):
    kl_o[...] = jnp.zeros_like(kl_o)
    for row in range(nr):
        base, half, length = seg(meta, row)
        first = lax.div(base, HALF)
        count = lax.div(half, HALF)

        def clear(chunk, unused, first=first):
            dk_o[first + chunk] = jnp.zeros((2 * HALF, B_S), F32)
            dv_o[first + chunk] = jnp.zeros((2 * HALF, B_S), F32)
            return unused

        lax.fori_loop(0, count, clear, 0)

        def one_block(step, unused, row=row, base=base, first=first, half=half, length=length, count=count):
            start = pl.multiple_of(base + step * BLOCK, HALF)
            inside = step * BLOCK + lax.broadcasted_iota(jnp.int32, (BLOCK, 1), 0) < half
            q_all = jnp.where(inside, q[pl.ds(start, BLOCK), :], jnp.zeros((), BF16))
            s_all = jnp.where(inside, sq[pl.ds(start, BLOCK), :], jnp.zeros((), BF16))
            m_all = jnp.where(inside, dmix[pl.ds(start, BLOCK), :], jnp.zeros((), BF16))
            flat = jnp.where(inside, delta[pl.ds(start, BLOCK), :], 0.0).T
            spot_q = step * BLOCK + lax.broadcasted_iota(jnp.int32, (1, BLOCK), 1)
            inside_q = spot_q < half
            live = inside_q & (meta[0] * half + spot_q < length)
            heads_s = [head_masked(s_all, h) for h in range(HEADS)]
            heads_m = [head_masked(m_all, h) for h in range(HEADS)]
            lines = jnp.concatenate([lse[lax.div(start, HALF)], lse[lax.div(start, HALF) + 1]], 1)
            lines_t = jnp.where(live, lines[:HEADS] - scale[2], 1e30)
            lines_s = jnp.where(inside_q, lines[HEADS:], 1e30)
            weight = jnp.where(live, scale[1], 0.0)
            offsets = [weight - jnp.sum(flat[h * HD_S : (h + 1) * HD_S], 0, keepdims=True) for h in range(HEADS)]
            acc_q[...] = jnp.zeros_like(acc_q)
            stack_s = jnp.concatenate(heads_s, 0)
            stack_m = jnp.concatenate(heads_m, 0)

            def value_grads(spot, slot):
                dv_o[spot] += dot(p_scr[slot], stack_m)

            def key_grads(spot, slot):
                dk_o[spot] += dot(g_scr[slot], stack_s)

            def scores(spot, h):
                return (
                    dot(k[spot, :, h * HD_T : (h + 1) * HD_T], q_all[:, h * HD_T : (h + 1) * HD_T], NT),
                    dot(sk[spot], heads_s[h], NT),
                    dot(sv[spot], heads_m[h], NT),
                )

            def prepare(spot, h):
                for n, value in enumerate(scores(spot, h)):
                    s_scr[n] = value

            def chunk_body(masked, chunk, kl):
                spot = first + chunk
                slot = lax.rem(chunk, 2)
                dead = dead_keys(meta, row, chunk) if masked else None

                def chain(h, made, kl):
                    u_t = made[0] * SCALE_T - lines_t[h : h + 1]
                    u_s = made[1] * SCALE_S - lines_s[h : h + 1]
                    if masked:
                        u_t = jnp.where(dead, -1e30, u_t)
                        u_s = jnp.where(dead, -1e30, u_s)
                    p_t = jnp.exp2(u_t)
                    p_s = jnp.exp2(u_s)
                    kl = kl + fold(p_t * (u_t - u_s))
                    low = (p_s * (made[2] + offsets[h]) - p_t).astype(BF16)
                    p_scr[slot, :, h * BLOCK : (h + 1) * BLOCK] = p_s.astype(BF16)
                    g_scr[slot, :, h * BLOCK : (h + 1) * BLOCK] = low
                    return low, kl

                def query_grad(h, low):
                    acc_q[h] += dot(skt[spot, h * HD_S : (h + 1) * HD_S, :], low)

                last = jnp.maximum(spot - 1, first)
                made = [s_scr[0], s_scr[1], s_scr[2]]
                ahead = scores(spot, 1)
                low, kl = chain(0, made, kl)
                value_grads(last, 1 - slot)
                made, ahead = ahead, scores(spot, 2)
                query_grad(0, low)
                low, kl = chain(1, made, kl)
                made, ahead = ahead, scores(spot, 3)
                query_grad(1, low)
                low, kl = chain(2, made, kl)
                key_grads(last, 1 - slot)
                made = ahead
                prepare(jnp.minimum(spot + 1, first + count - 1), 0)
                query_grad(2, low)
                low, kl = chain(3, made, kl)
                query_grad(3, low)
                return kl

            p_scr[1] = jnp.zeros_like(p_scr[1])
            g_scr[1] = jnp.zeros_like(g_scr[1])
            prepare(first, 0)
            kl = chunk_loops(meta, row, chunk_body, jnp.zeros((8, BLOCK), F32))
            value_grads(first + count - 1, lax.rem(count - 1, 2))
            key_grads(first + count - 1, lax.rem(count - 1, 2))
            kl_o[0] += kl
            kl_o[1, 0:1] += jnp.where(live, -HEADS * scale[1] * scale[2], 0.0)
            dq_o[pl.ds(start, BLOCK), :] = acc_q[...].reshape(B_S, BLOCK).T
            return unused

        lax.fori_loop(0, lax.div(half + BLOCK - 1, BLOCK), one_block, 0)


def attend_back(nr, meta, scale, *ins):
    cap = ins[0].shape[0]
    nblk = cap // HALF
    outs = [
        jax.ShapeDtypeStruct((cap, B_S), F32),
        jax.ShapeDtypeStruct((nblk, 2 * HALF, B_S), F32),
        jax.ShapeDtypeStruct((nblk, 2 * HALF, B_S), F32),
        jax.ShapeDtypeStruct((2, 8, BLOCK), F32),
    ]
    return pl.pallas_call(
        functools.partial(back_body, nr),
        grid_spec=pltpu.PrefetchScalarGridSpec(
            num_scalar_prefetch=2,
            grid=(1,),
            in_specs=[whole(a.shape) for a in ins],
            out_specs=[whole(a.shape) for a in outs],
            scratch_shapes=[
                pltpu.VMEM((HEADS, HD_S, BLOCK), F32),
                pltpu.VMEM((2, 2 * HALF, HEADS * BLOCK), BF16),
                pltpu.VMEM((2, 2 * HALF, HEADS * BLOCK), BF16),
                pltpu.VMEM((3, 2 * HALF, BLOCK), F32),
            ],
        ),
        out_shape=outs,
        compiler_params=params(),
        name="attend_back",
    )(meta, scale, *ins)


def finish_body(
    meta, scale, dq, dk, dv, pk, pv, datt, npre, nbf, inputs, attention, ssc, gcomb, s128, s512, kl, late_o, t128, t384
):
    step = pl.program_id(0)

    @pl.when(step == 0)
    def _():
        for ref in (late_o, t128, t384):
            ref[...] = jnp.zeros_like(ref)

    inside = step * BLOCK + lax.broadcasted_iota(jnp.int32, (BLOCK, 1), 0) < meta[1]
    d_q = dq[...] * KEY_SCALE
    d_k = (dk[...].reshape(BLOCK, B_S) + pk[...].reshape(BLOCK, B_S).astype(F32)) * KEY_SCALE
    d_v = dv[...].reshape(BLOCK, B_S) + pv[...].reshape(BLOCK, B_S).astype(F32)
    d_all = jnp.where(inside, jnp.concatenate([d_q, d_k, d_v], 1), 0.0).astype(BF16)
    t384[...] += fold(d_all.astype(F32))
    late_o[B_S : 2 * B_S, B_S:] += dot(nbf[...], d_all, TN)
    d_narrow = datt[...] + dot(d_all, attention[...].astype(BF16), NT)
    t128[0] += fold(d_narrow * npre[...])
    t128[1] += fold(d_narrow)
    d_enter = (d_narrow * spart(ssc, 1)).astype(BF16)
    t128[2] += fold(d_enter.astype(F32))
    late_o[:B_S, :] += dot(d_enter, inputs[...], TN)

    @pl.when(step == meta[2] - 1)
    def _():
        line = lambda v: jnp.sum(v, 0, keepdims=True)
        join = lambda items: jnp.concatenate([line(v) for v in items], 1)
        late_o[B_S : 2 * B_S, :B_S] = gcomb[...]
        loss = jnp.sum(line(s512[0]), 1, keepdims=True) * (scale[0] / D_S) + LN2 * (
            jnp.sum(line(kl[0]), 1, keepdims=True) + jnp.sum(line(kl[1]), 1, keepdims=True)
        )
        items = [
            join([t128[2], t128[0], t128[1], t384[:, :B_S]]),
            join([t384[:, 2 * B_S :], s128[14], s128[12], s128[13]]),
        ]
        items += [line(s512[4 + n]) for n in range(NFFN)]
        items += [join([s128[8 + n] for n in range(NFFN)]), join([s128[n] for n in range(NFFN)])]
        items += [join([s128[4 + n] for n in range(NFFN)]), line(s512[3]), line(s512[1]), line(s512[2])]
        items += [jnp.broadcast_to(loss, (1, D_S)), jnp.zeros((3, D_S), F32)]
        late_o[2 * B_S : 2 * B_S + 16, :] = jnp.concatenate(items, 0)


def finish(meta, scale, dq, dk, dv, pk, pv, datt, npre, nbf, inputs, attention, ssc, gcomb, s128, s512, kl):
    cap = dq.shape[0]
    mine = pl.BlockSpec((2, 1, HALF, B_S), lambda i, meta, *s: (at(i, meta), 0, 0, 0))
    peer = pl.BlockSpec((2, HALF, B_S), lambda i, meta, *s: (at(i, meta), 0, 0))
    fixed = (attention, ssc, gcomb, s128, s512, kl)
    return pl.pallas_call(
        when_live(finish_body),
        grid_spec=pltpu.PrefetchScalarGridSpec(
            num_scalar_prefetch=2,
            grid=(cap // BLOCK,),
            in_specs=[rows(B_S), mine, mine, peer, peer, rows(B_S), rows(B_S), rows(B_S), rows(D_S)]
            + [whole(a.shape) for a in fixed],
            out_specs=whole((LATE, D_S)),
            scratch_shapes=[pltpu.VMEM((3, 8, B_S), F32), pltpu.VMEM((8, 3 * B_S), F32)],
        ),
        out_shape=jax.ShapeDtypeStruct((LATE, D_S), F32),
        compiler_params=params(),
        name="finish",
    )(meta, scale, dq, dk, dv, pk, pv, datt, npre, nbf, inputs, *fixed)


class Line:
    def __init__(self, size, spot, device):
        self.size, self.spot, self.device = size, spot, device


def lines_of(n_dp, n_seq):
    dp, seq = lax.axis_index("dp"), lax.axis_index("seq")
    n_low = line_sizes(n_dp, n_seq)[2]
    low, high = lax.rem(dp, n_low), lax.div(dp, n_low)
    core, y = lax.rem(seq, 2), lax.div(seq, 2)
    return (
        Line(2, core, lambda j: {"dp": dp, "seq": y * 2 + j}),
        Line(n_seq // 2, y, lambda j: {"dp": dp, "seq": j * 2 + core}),
        Line(n_low, low, lambda j: {"dp": high * n_low + j, "seq": seq}),
        Line(n_dp // n_low, high, lambda j: {"dp": j * n_low + low, "seq": seq}),
    )


def line_sizes(n_dp, n_seq):
    n_low = 2 if n_dp == 8 else 4
    return (2, n_seq // 2, n_low, n_dp // n_low)


ORDERS = ((0, 1, 2, 3), (0, 2, 1, 3))


def sum_parts(n_dp, n_seq, needed):
    sizes = line_sizes(n_dp, n_seq)
    unit = 8
    for size in sizes:
        unit *= size
    plans = []
    for order in ORDERS:
        length, plan = unit, []
        for axis in order:
            length //= sizes[axis]
            plan.append((axis, length))
        plans.append(plan)
    count = -(-needed // unit)
    return unit, count, [plans[part % 2] for part in range(count)]


def sum_body(n_dp, n_seq, early, late, out, *scratch):
    work, send_sem, recv_sem = scratch[-3], scratch[-2], scratch[-1]
    lines = lines_of(n_dp, n_seq)
    sizes = line_sizes(n_dp, n_seq)
    needed = early.shape[0] + late.shape[0]
    unit, count, plans = sum_parts(n_dp, n_seq, needed)

    barrier = pltpu.get_barrier_semaphore()
    met = 0
    for line, size in zip(lines, sizes, strict=True):
        for step in range(1, size):
            pl.semaphore_signal(
                barrier, inc=1, device_id=line.device(lax.rem(line.spot + step, size)), device_id_type=pl.DeviceIdType.MESH
            )
            met += 1
    work[: early.shape[0], :] = early[...]
    work[early.shape[0] : needed, :] = late[...]
    if unit * count > needed:
        work[needed:, :] = jnp.zeros((unit * count - needed, D_S), F32)
    pl.semaphore_wait(barrier, met)

    number = [0]

    def remote(src, dst, line, step, size):
        n = number[0]
        number[0] += 1
        copy = pltpu.make_async_remote_copy(
            src_ref=src, dst_ref=dst, send_sem=send_sem.at[n], recv_sem=recv_sem.at[n],
            device_id=line.device(lax.rem(line.spot + step, size)), device_id_type=pl.DeviceIdType.MESH,
        )
        copy.start()
        return copy

    starts = [[part * unit] for part in range(count)]
    flying = [None] * count
    levels = len(ORDERS[0])

    def launch(part, turn):
        if turn < levels:
            axis, sub = plans[part][turn]
            line, size = lines[axis], sizes[axis]
            copies = []
            for step in range(1, size):
                target = lax.rem(line.spot + step, size)
                start = pl.multiple_of(starts[part][turn] + target * sub, 8)
                buffer = scratch[part * levels + turn].at[step - 1]
                copies.append(remote(work.at[pl.ds(start, sub), :], buffer, line, step, size))
        else:
            level = 2 * levels - 1 - turn
            axis, sub = plans[part][level]
            line, size = lines[axis], sizes[axis]
            piece = out.at[pl.ds(starts[part][level + 1], sub), :]
            copies = [remote(piece, piece, line, step, size) for step in range(1, size)]
        flying[part] = copies

    def land(part, turn):
        for copy in flying[part]:
            copy.wait()
        if turn < levels:
            axis, sub = plans[part][turn]
            line, size = lines[axis], sizes[axis]
            start = pl.multiple_of(starts[part][turn] + line.spot * sub, 8)
            value = work[pl.ds(start, sub), :]
            for step in range(1, size):
                value = value + scratch[part * levels + turn][step - 1]
            (out if turn == levels - 1 else work)[pl.ds(start, sub), :] = value
            starts[part].append(start)

    waves = -(-count // 2)
    for wave in range(2 * levels + waves):
        for part in range(count):
            turn = wave - part // 2
            if 0 < turn <= 2 * levels:
                land(part, turn - 1)
            if 0 <= turn < 2 * levels:
                launch(part, turn)


def sum_all(n_dp, n_seq, early, late):
    sizes = line_sizes(n_dp, n_seq)
    unit, count, plans = sum_parts(n_dp, n_seq, early.shape[0] + late.shape[0])
    buffers = [pltpu.VMEM((sizes[axis] - 1, sub, D_S), F32) for plan in plans for axis, sub in plan]
    copies = 2 * count * sum(size - 1 for size in sizes)
    return pl.pallas_call(
        functools.partial(sum_body, n_dp, n_seq),
        in_specs=[pl.BlockSpec(memory_space=pltpu.VMEM)] * 2,
        out_specs=pl.BlockSpec(memory_space=pltpu.VMEM),
        out_shape=jax.ShapeDtypeStruct((unit * count, D_S), F32),
        scratch_shapes=buffers
        + [
            pltpu.VMEM((unit * count, D_S), F32),
            pltpu.SemaphoreType.DMA((copies,)),
            pltpu.SemaphoreType.DMA((copies,)),
        ],
        compiler_params=params(collective_id=1, has_side_effects=True),
        name="sum_all",
    )(early, late)


FIRST_FIX = 1.0 / (1.0 - BETA_ONE**STEP)
SECOND_FIX = 1.0 / (1.0 - BETA_TWO**STEP)


def adam_body(grads, *refs):
    weights, moments, squares = refs[:7], refs[7:14], refs[14:21]
    new_w, new_m, new_s, norm_o = refs[21:28], refs[28:35], refs[35:42], refs[42]
    top = EARLY + 2 * B_S
    total = jnp.zeros((8, D_S), F32)
    for start in range(0, top, B_S):
        part = grads[start : start + B_S, :]
        total = total + fold(part * part)
    extra = grads[top : top + 12, :]
    square = jnp.sum(total, 0, keepdims=True) + jnp.sum(extra * extra, 0, keepdims=True)
    grad_norm = jnp.sqrt(jnp.sum(square, 1, keepdims=True))
    norm_o[0:1, :] = jnp.broadcast_to(grad_norm, (1, HALF))
    norm_o[1:2, :] = grads[top + 12 : top + 13, :HALF]
    factor = CLIP / jnp.maximum(grad_norm, CLIP)

    def update(n, where, grad):
        g = grad * factor
        weight = weights[n][where]
        first = BETA_ONE * moments[n][where] + (1.0 - BETA_ONE) * g
        second = BETA_TWO * squares[n][where] + (1.0 - BETA_TWO) * g * g
        change = (first * FIRST_FIX) / (jnp.sqrt(second * SECOND_FIX) + ADAM_EPS)
        if n < 6:
            change = change + DECAY * weight
        new_w[n][where] = weight - LRATE * change
        new_m[n][where] = first
        new_s[n][where] = second

    every = (slice(None), slice(None))
    update(0, every, grads[EARLY : EARLY + B_S, :].T)
    update(1, every, grads[EARLY + B_S : top, B_S:])
    update(2, every, grads[EARLY + B_S : top, :B_S])
    for n in range(NFFN):
        update(3, n, grads[n * B_S : (n + 1) * B_S, :])
        update(4, n, grads[(NFFN + n) * B_S : (NFFN + n + 1) * B_S, :].T)
    update(5, every, grads[2 * NFFN * B_S : EARLY, :])
    for n in range(12):
        update(6, (slice(0, 1), slice(n * D_S, (n + 1) * D_S)), grads[top + n : top + n + 1, :])


def adam(grads, weights, moments, squares):
    like = [jax.ShapeDtypeStruct(w.shape, F32) for w in weights]
    outs = like * 3 + [jax.ShapeDtypeStruct((2, HALF), F32)]
    return pl.pallas_call(
        adam_body,
        in_specs=[pl.BlockSpec(memory_space=pltpu.VMEM)] * 22,
        out_specs=[pl.BlockSpec(memory_space=pltpu.VMEM)] * 22,
        out_shape=outs,
        compiler_params=params(),
        name="adam",
    )(grads, *weights, *moments, *squares)


def shards(
    tokens, segment_ends, word_table, trigram_conv, position_table, segment_table, embed_scalars,
    teacher_enter, teacher_attention, teacher_combine, teacher_expand, teacher_reduce, teacher_leave, teacher_scalars,
    narrowing, attention, combining, expanding, reducing, widening, scalars, *state,
):
    micros, rows_here, local = tokens.shape
    n_dp, n_seq = lax.axis_size("dp"), lax.axis_size("seq")
    full = local * n_seq
    half_cap = full // 2
    n_rows = micros * rows_here * n_dp
    n_chips = n_dp * n_seq // 2
    nr = n_rows // n_chips
    cap = nr * half_cap
    seq = lax.axis_index("seq")
    core = seq % 2
    chip = lax.axis_index("dp") * (n_seq // 2) + seq // 2
    swap = [(i, i ^ 1) for i in range(n_seq)]

    token_lines = micros * rows_here * local // HALF
    ends_line = jnp.pad(segment_ends.reshape(1, -1), ((0, 0), (0, HALF - micros * rows_here * 2)))
    told = share(n_dp, n_seq, jnp.concatenate([tokens.reshape(token_lines, HALF), ends_line], 0))
    if n_seq == 4:
        side = lax.ppermute(position_table, "seq", swap)
        cross = lax.ppermute(position_table, "seq", [(i, i ^ 2) for i in range(4)])
        corner = lax.ppermute(cross, "seq", swap)
        places = jnp.stack([position_table, side, cross, corner])
        turn = seq
    else:
        places = lax.all_gather(position_table, "seq", axis=0)
        turn = jnp.int32(0)

    ends = told[:, token_lines, : micros * rows_here * 2].reshape(n_dp, n_seq, micros * rows_here, 2)[:, 0]
    ends = ends.reshape(n_rows, 2)
    lengths = ends[:, 1]
    count = jnp.sum(lengths.astype(F32))
    order = jnp.arange(n_rows, dtype=jnp.int32)
    ahead = (lengths[None, :] > lengths[:, None]) | (
        (lengths[None, :] == lengths[:, None]) & (order[None, :] < order[:, None])
    )
    rank = jnp.sum(ahead.astype(jnp.int32), 1)
    picks = []
    for j in range(nr):
        wanted = j * n_chips + (chip if j % 2 == 0 else n_chips - 1 - chip)
        hit = (rank == wanted).astype(jnp.int32)
        picks.append((jnp.sum(hit * order), jnp.sum(hit * ends[:, 0]), jnp.sum(hit * lengths)))
    halves = [(length + 255) // 256 * HALF for _, _, length in picks]
    bases = [sum(halves[:j], jnp.int32(0)) for j in range(nr)]
    slots = sum(halves, jnp.int32(0))
    meta = [core, slots, (slots + BLOCK - 1) // BLOCK]
    for j in range(nr):
        meta += [bases[j], halves[j], picks[j][2]]
    meta += [pick[1] for pick in picks] + [turn]
    meta = jnp.stack([jnp.asarray(v, jnp.int32) for v in meta])
    scale_back = 1.0 / count
    scale = jnp.stack([scale_back, scale_back / HEADS, jnp.log2(scale_back / HEADS)])

    ids = jnp.zeros((cap,), jnp.int32)
    edges = []
    every = told[:, :token_lines].reshape(n_dp, n_seq, micros * rows_here, local)
    for j in range(nr):
        owner, inner = picks[j][0] // (micros * rows_here), picks[j][0] % (micros * rows_here)
        line = lax.dynamic_slice(every, (owner, 0, inner, 0), (1, n_seq, 1, local)).reshape(full)
        first = core * halves[j]
        edges += [
            lax.dynamic_slice(line, (jnp.maximum(first - 1, 0),), (1,)),
            lax.dynamic_slice(line, (jnp.minimum(first + halves[j], full - 1),), (1,)),
        ]
        ids = lax.dynamic_update_slice(ids, lax.dynamic_slice(line, (first,), (half_cap,)), (bases[j],))
    ids = jnp.concatenate([ids] + edges + [jnp.zeros((16 - 2 * nr,), jnp.int32)])
    words = word_table.at[ids].get(mode="promise_in_bounds")
    inputs = embed(nr, full, meta, words, places, trigram_conv, segment_table, embed_scalars)
    peer_inputs = lax.ppermute(inputs, "seq", swap)

    tsc = teacher_scalars.reshape(1, -1)
    ssc = scalars.reshape(1, -1)
    weights = (teacher_enter, teacher_attention, tsc, narrowing, attention, ssc)
    front, q, k, vt, npre, nbf, sq, sk, skt, sv, svt = project(True, meta, inputs, weights)
    k, vt, sk, skt, sv, svt = project(False, meta, peer_inputs, weights, (k, vt, sk, skt, sv, svt))
    nblk = k.shape[0]
    k3 = k.reshape(nblk, 2 * HALF, D_T)
    sk3 = sk.reshape(nblk, 2 * HALF, B_S)
    sv3 = sv.reshape(nblk, 2 * HALF, B_S)
    mixed, smixed, lse = attend(nr, meta, q, k3, vt, sq, sk3, svt)
    target = teacher_tail(
        meta, mixed, front, inputs, (teacher_combine, teacher_expand, teacher_reduce, teacher_leave, tsc)
    )
    dmix, datt, delta, early, g_comb, s128, s512 = student_tail(
        nr, meta, scale, smixed, npre, inputs, target, (combining, expanding, reducing, widening, ssc)
    )
    dq, dk, dv, kl = attend_back(nr, meta, scale, q, k3, sq, sk3, skt, sv3, dmix, delta, lse)
    dk = dk.reshape(nblk, 2, HALF, B_S)
    dv = dv.reshape(nblk, 2, HALF, B_S)
    pk = lax.ppermute(dk[:, 1].astype(BF16), "seq", swap)
    pv = lax.ppermute(dv[:, 1].astype(BF16), "seq", swap)
    late = finish(meta, scale, dq, dk, dv, pk, pv, datt, npre, nbf, inputs, attention, ssc, g_comb, s128, s512, kl)
    grads = sum_all(n_dp, n_seq, early, late)
    flat = lambda items: list(items[:6]) + [items[6].reshape(1, -1)]
    outs = adam(
        grads,
        [narrowing, attention, combining, expanding, reducing, widening, ssc],
        flat(state[:7]),
        flat(state[7:14]),
    )
    final = []
    for n in range(3):
        final += list(outs[7 * n : 7 * n + 6]) + [outs[7 * n + 6].reshape(-1)]
    return tuple(final) + (outs[21][1, :1], outs[21][0, :1])


def solution(mesh):
    specs = [P()] * 35
    specs[0] = P(None, "dp", "seq")
    specs[1] = P(None, "dp", None)
    specs[4] = P("seq", None)
    return jax.shard_map(
        shards, mesh=mesh, in_specs=tuple(specs), out_specs=tuple([P()] * 23), check_vma=False
    )
```
